32 devices in a mesh: expert: 4 (over y, x), dp: 8 (over z, core).
Axes of the slice: x: 2, y: 2, z: 4, core: 2. Of those that a mesh axis runs over, the one named last changes fastest.
Arguments:
- tokens: bfloat16 [2, 4096, 1280], P(None, ('expert', 'dp')), may hold values from -6 to 6
- modality: int32 [2, 4096], P(None, ('expert', 'dp')), may hold values from 0 to 1, as said below
- routes: int32 [2, 4096, 1], P(None, ('expert', 'dp')), may hold values from 0 to 3; in each aligned block of 128 rows (0 to 127, 128 to 255, ..., all dimensions but the last counted through in order) at most 64 rows name the same one
- router: bfloat16 [1280, 4], replicated, may hold values from -0.15625 to 0.15625
- w_in: bfloat16 [4, 1280, 5120], P('expert', 'dp'), may hold values from -0.15625 to 0.15625
- w_out: bfloat16 [4, 5120, 1280], P('expert', 'dp'), may hold values from -0.078125 to 0.078125
Outputs:
- mixed: bfloat16 [2, 4096, 1280], P(None, ('expert', 'dp'))
- load: float32 [2, 2, 4], replicated
The draws below stay inside these ranges and needn't reach their ends.
Inputs may be any that keep to these rules, and one draw needn't show every extreme that they name: `routes`: among the 128 tokens of one micro-batch on one device (aligned blocks of 128 rows), at most 64 are routed to any one expert. `modality`: in every aligned block of 128 tokens of a micro-batch, the number of text tokens lies between 32 and 96.
All inputs are finite; a program needn't handle non-finite values.
Results may differ from the reference program's by a relative error of at most 0.0057.
Values may be sent and summed in bfloat16 or wider, within the bound.
A program may use at most 192 MiB of HBM per device.

```python
import math
import jax
import jax.numpy as jnp
import numpy as np
from jax import lax

D = 1280
FF = 5120
MB = 2
TOK_MB = 128
EXPERTS = 4
CAP = 64
TOKENS = 4096


def draw_modality(key, part):
    n_blocks = TOKENS // TOK_MB
    scores = jax.random.randint(key, (MB, n_blocks, TOK_MB), 0, 1 << 20) * TOK_MB + jnp.arange(TOK_MB, dtype=jnp.int32)
    order = jnp.argsort(scores, axis=-1)
    ranked = jnp.argsort(order, axis=-1)
    texts = TOK_MB // 4 + TOK_MB // 2 * jnp.arange(n_blocks, dtype=jnp.int32) // max(n_blocks - 1, 1)
    return (ranked < texts[None, :, None]).astype(jnp.int32).reshape(MB, TOKENS)


def level_of(key, shape, cuts, least, largest):
    def one(axis_at, shards_of):
        heights = jax.random.uniform(jax.random.fold_in(jax.random.fold_in(key, 6), axis_at), (shards_of,), jnp.float32, least / len(cuts), largest / len(cuts))
        return jnp.repeat(jnp.exp(heights), shape[axis_at] // shards_of).reshape((-1,) + (1,) * (len(shape) - axis_at - 1))

    gain = one(*cuts[0])
    for cut in cuts[1:]:
        gain = gain * one(*cut)
    return gain


def shared_out(key, own, number, rows, count, top, reach, skew):
    order = jax.random.permutation(key, count)
    crowded, common = load_shares(count, rows * top, reach, skew, True), load_shares(count, rows * top, reach, skew, False)
    places = jnp.arange(count)

    def named(sizes, offset_by):
        used = int((sizes > 0).sum())
        fixed = max(1, used // 4)
        shifted = fixed + (places - fixed + offset_by * (used - fixed)) % max(1, count - fixed)
        return jnp.zeros((count,), jnp.int32).at[order[jnp.where(places < fixed, places, shifted)]].set(jnp.asarray(sizes, jnp.int32))

    sizes = jnp.where(number % 4 == 0, named(crowded, number // 4), named(common, number - number // 4 - 1))
    mixed = jax.random.permutation(jax.random.fold_in(own, 3), count)
    donor, sink = mixed[0:count // 2 * 2:2], mixed[1:count // 2 * 2:2]
    room = jnp.minimum(sizes[donor] - 1, reach - sizes[sink]) // 2
    room = jnp.where((donor == order[0]) | (sink == order[0]) | (sizes[sink] == 0), 0, jnp.maximum(room, 0))
    shifted = jax.random.randint(jax.random.fold_in(own, 4), (count // 2,), 0, 1 << 20) % (room + 1)
    sizes = sizes.at[donor].add(-shifted).at[sink].add(shifted)
    items = jnp.searchsorted(jnp.cumsum(sizes), jnp.arange(rows * top), side="right").astype(jnp.int32)
    listing = items.reshape(top, rows).T
    listing = listing[jax.random.permutation(jax.random.fold_in(own, 1), rows)]
    offset_by = jax.random.randint(jax.random.fold_in(own, 2), (rows, 1), 0, top)
    return jnp.take_along_axis(listing, (jnp.arange(top)[None, :] + offset_by) % top, axis=1)


def load_shares(number_of, total, most, skew, full):
    portions = [(1 << 20) // math.isqrt(grade ** skew) + 1 for grade in range(1, number_of + 1)]
    largest = most if full else min(most, max(-(-total // number_of), total * portions[0] // sum(portions)))
    least = 1 if total - largest >= number_of - 1 else 0
    given, rest = [largest] + [least] * (number_of - 1), total - largest - least * (number_of - 1)
    while rest > 0:
        candidates = [i for i in range(1, number_of) if given[i] < largest] or [i for i in range(1, number_of) if given[i] < most]
        pool, budget = sum([portions[i] for i in candidates]), rest
        for i in candidates:
            extra = min(most - given[i], max(1, budget * portions[i] // pool), rest)
            given[i] = given[i] + extra
            rest = rest - extra
    return np.array(given)


def gaussian(stream_key, shape, deviation, reach, pieces=(), kind=jnp.bfloat16):
    drawn = jax.random.normal(stream_key, shape, jnp.float32) * deviation
    if len(pieces) > 0:
        drawn = level_of(stream_key, shape, pieces, -0.22, 0.18) * drawn
    return jnp.clip(drawn, min=-reach, max=reach).astype(kind)


def setup_inputs(seed: int = 0) -> dict:
    streams_of = jax.random.split(jax.random.key(seed), 7)
    tokens = gaussian(streams_of[0], (MB, TOKENS, D), 1.0, 6.0, ((1, 32),))
    modality = draw_modality(jax.random.fold_in(streams_of[6], 71), 0)
    routes_keys = jax.random.split(jax.random.fold_in(streams_of[2], 1), MB * TOKENS // TOK_MB)
    routes_turns = jax.random.permutation(jax.random.fold_in(streams_of[2], 3), MB * TOKENS // TOK_MB)
    routes = jax.vmap(lambda own, number: shared_out(jax.random.fold_in(streams_of[2], 2), own, number, TOK_MB, EXPERTS, 1, CAP, 2))(routes_keys, routes_turns).reshape((MB, TOKENS, 1))
    router = gaussian(streams_of[3], (D, EXPERTS), D ** -0.5, 0.15625)
    w_in = gaussian(streams_of[4], (EXPERTS, D, FF), D ** -0.5, 0.15625, ((0, 4), (1, 8)))
    w_out = gaussian(streams_of[5], (EXPERTS, FF, D), FF ** -0.5, 0.078125, ((0, 4), (1, 8)))
    return dict(tokens=tokens, modality=modality, routes=routes, router=router, w_in=w_in, w_out=w_out)


def expert_mlp(operands):
    rows_in, weight_in, weight_out = operands
    pre_act = jnp.dot(rows_in, weight_in, preferred_element_type=jnp.float32)
    hidden = jax.nn.gelu(pre_act, approximate=True).astype(jnp.bfloat16)
    return jnp.dot(hidden, weight_out, preferred_element_type=jnp.float32).astype(jnp.bfloat16)


def reference(tokens, modality, routes, router, w_in, w_out):
    blocks = TOKENS // TOK_MB
    slot_bound = blocks * CAP
    mixed_list = []
    counts = jnp.zeros((2, EXPERTS), jnp.float32)
    prob_sums = jnp.zeros((2, EXPERTS), jnp.float32)
    modal_counts = jnp.zeros((2,), jnp.float32)
    for micro in range(MB):
        micro_tokens = tokens[micro]
        expert_ids = routes[micro, :, 0].astype(jnp.int32)
        logits = jnp.dot(micro_tokens, router, preferred_element_type=jnp.float32)
        onehot = (expert_ids[:, None] == jnp.arange(EXPERTS, dtype=jnp.int32)[None, :]).astype(jnp.float32)
        gating = jax.nn.sigmoid(jnp.sum(logits * onehot, axis=-1))
        running = jnp.cumsum(onehot.reshape(blocks, TOK_MB, EXPERTS), axis=1).reshape(TOKENS, EXPERTS)
        slot_pos = (jnp.sum(running * onehot, axis=-1) - 1.0).astype(jnp.int32)
        device = (jnp.arange(TOKENS, dtype=jnp.int32) // TOK_MB).astype(jnp.int32)
        position = (expert_ids * slot_bound + device * CAP + slot_pos).astype(jnp.int32)
        buffer = jnp.zeros((EXPERTS * slot_bound, D), jnp.bfloat16).at[position].set(micro_tokens)
        buffer = buffer.reshape(EXPERTS, slot_bound, D)
        result = lax.map(expert_mlp, (buffer, w_in, w_out)).reshape(EXPERTS * slot_bound, D)
        scaled = result[position].astype(jnp.float32) * gating[:, None]
        mixed_list.append(scaled.astype(jnp.bfloat16))
        exps = jnp.exp(logits)
        router_probs = exps / jnp.sum(exps, axis=-1, keepdims=True)
        modal_hot = (modality[micro][:, None] == jnp.arange(2, dtype=jnp.int32)[None, :]).astype(jnp.float32)
        counts = counts + jnp.dot(modal_hot.T, onehot, precision=lax.Precision.HIGHEST)
        prob_sums = prob_sums + jnp.dot(modal_hot.T, router_probs, precision=lax.Precision.HIGHEST)
        modal_counts = modal_counts + jnp.sum(modal_hot, axis=0)
    load = jnp.stack([EXPERTS * counts / modal_counts[:, None], EXPERTS * prob_sums / modal_counts[:, None]])
    return jnp.stack(mixed_list), load
```

```python
import functools

import jax
import jax.numpy as jnp
from jax import lax
from jax.experimental import pallas as pl
from jax.experimental.pallas import tpu as pltpu
from jax.sharding import PartitionSpec as P

MESH = pl.DeviceIdType.MESH
BF16 = jnp.bfloat16
F32 = jnp.float32


def layer_kernel(
    experts,
    ranks,
    splits,
    tokens_ref,
    routes_ref,
    modality_ref,
    router_ref,
    w_in_ref,
    w_out_ref,
    mixed_ref,
    load_ref,
    tok_far,
    routes_far,
    slot_row,
    back_hot,
    gate,
    sums,
    stats_e,
    stats_d,
    win,
    wout,
    xs,
    xr,
    acc,
    hid,
    ys,
    yr,
    zs,
    zr,
    tok_sem,
    routes_sem,
    stat_sem,
    far_sem,
    in_send,
    in_recv,
    out_send,
    out_recv,
    x_sem,
    x_own,
    y_sem,
    y_own,
    z_send,
    z_recv,
):
    micro, tok, width = tokens_ref.shape
    in_rows, ff = w_in_ref.shape
    out_rows = w_out_ref.shape[0]
    half_ff = ff // 2
    pieces, tile_w = zr.shape[0], zr.shape[3]
    cap = xs.shape[3]
    slots_all = experts * cap
    side_rows = experts * micro * cap
    e = lax.axis_index("expert")
    p = lax.axis_index("dp")
    z, c = p // 2, p % 2
    chips = ranks // 2
    group = chips // 2
    pairs = group // 2
    h = z // group
    zl = z % group
    mate = z * 2 + (1 - c)
    inner = (z % 2) == (1 - h)
    outer = (z % 2) == h
    role = (z + h) % 2

    def far_rank(t, which, core):
        pair = (1 - h) * pairs + ((z // 2) % pairs + t) % pairs
        return (pair * 2 + (1 - h + which) % 2) * 2 + core

    far_in = far_rank(0, 1, c)
    far_out = far_rank(0, 0, c)

    def peer(k):
        return (h * group + (zl + k) % group) * 2 + c

    def place(k, core):
        return ((zl + k) % group) * 2 + core

    barrier = pltpu.get_barrier_semaphore()

    def greet_e(k, carry):
        pl.semaphore_signal(
            barrier, inc=1, device_id=((e + k) % experts, p), device_id_type=MESH
        )
        return carry

    def greet_d(k, carry):
        pl.semaphore_signal(barrier, inc=1, device_id=(e, (p + k) % ranks), device_id_type=MESH)
        return carry

    lax.fori_loop(1, experts, greet_e, 0)
    lax.fori_loop(1, ranks, greet_d, 0)

    def remote(src, dst, send, recv, dp=None, expert=None):
        return pltpu.make_async_remote_copy(
            src_ref=src,
            dst_ref=dst,
            send_sem=send,
            recv_sem=recv,
            device_id=(e if expert is None else expert, p if dp is None else dp),
            device_id_type=MESH,
        )

    def arrive(ref, sem):
        pltpu.make_async_copy(ref, ref, sem).wait()

    def win_rows(q, start=0, size=half_ff):
        return win.at[pl.ds(pl.multiple_of(q * in_rows, 16), in_rows), pl.ds(start, size)]

    def wout_rows(r, piece):
        return wout.at[
            pl.ds(pl.multiple_of(r * out_rows, 16), out_rows), pl.ds(piece * tile_w, tile_w)
        ]

    def cols(which, start=0, size=half_ff):
        return w_in_ref.at[:, pl.ds(pl.multiple_of(which * half_ff + start, 128), size)]

    def w_out_piece(piece):
        return w_out_ref.at[:, pl.ds(piece * tile_w, tile_w)]

    tok_copy = remote(
        tokens_ref, tok_far.at[role], tok_sem.at[0, 0], tok_sem.at[1, role], dp=far_in
    )
    routes_copy = remote(
        routes_ref, routes_far.at[role], routes_sem.at[0, 0], routes_sem.at[1, role], dp=far_in
    )
    far_copies = [
        remote(cols(1 - h, at, size), win_rows(p, at, size), far_sem.at[j], in_recv.at[p, j], dp=far_in)
        for j, (at, size) in enumerate(splits)
    ]
    near_peers = [
        remote(cols(h), win_rows(p), in_send.at[p, 0, k], in_recv.at[p, 0], dp=peer(k))
        for k in range(1, group)
    ]
    near_mate = remote(cols(h), win_rows(p), in_send.at[p, 0, 0], in_recv.at[p, 0], dp=mate)
    own_in = pltpu.make_async_copy(cols(h), win_rows(p), in_recv.at[p, 0])
    mine = place(0, c)
    out_peers = [
        [
            remote(
                w_out_piece(i), wout_rows(mine, i), out_send.at[mine, i, k], out_recv.at[mine, i],
                dp=peer(k),
            )
            for k in range(1, group)
        ]
        for i in range(pieces)
    ]
    out_mate = [
        remote(
            w_out_piece(i), wout_rows(mine, i), out_send.at[mine, i, 0], out_recv.at[mine, i], dp=mate
        )
        for i in range(pieces)
    ]
    own_out = [
        pltpu.make_async_copy(w_out_piece(i), wout_rows(mine, i), out_recv.at[mine, i])
        for i in range(pieces)
    ]

    def pass_near(k):
        q = peer(k)
        return remote(win_rows(q), win_rows(q), in_send.at[q, 0, 0], in_recv.at[q, 0], dp=mate)

    def pass_far(q, j, k):
        at, size = splits[j]
        rows = win_rows(q, at, size)
        to = mate if k == 0 else peer(k)
        return remote(rows, rows, in_send.at[q, j, k], in_recv.at[q, j], dp=to)

    def pass_out(k, i):
        r = place(k, c)
        rows = wout_rows(r, i)
        return remote(rows, rows, out_send.at[r, i, 0], out_recv.at[r, i], dp=mate)

    pl.semaphore_wait(barrier, experts + ranks - 2)

    early = pieces - 2
    routes_copy.start()
    tok_copy.start()

    @pl.when(inner)
    def _():
        for copy in far_copies:
            copy.start()
        for copy in near_peers:
            copy.start()
        for i in range(early):
            for copy in out_peers[i]:
                copy.start()

    @pl.when(outer)
    def _():
        for copy in near_peers:
            copy.start()
        for copy in far_copies:
            copy.start()
        for i in range(pieces):
            for copy in out_peers[i]:
                copy.start()

    near_mate.start()
    own_in.start()
    for i in range(pieces):
        out_mate[i].start()
        own_out[i].start()

    rows_e = max(experts, 8)

    def hot_of(row):
        at = lax.broadcasted_iota(jnp.int32, (rows_e, tok), 0)
        return jnp.where(at == row, 1.0, 0.0)

    def spread(row):
        return jnp.broadcast_to(row, (tok, tok)).T

    def assign(side, ref):
        ahead = lax.broadcasted_iota(jnp.int32, (tok, tok), 0) < lax.broadcasted_iota(
            jnp.int32, (tok, tok), 1
        )
        ahead = jnp.where(ahead, 1.0, 0.0).astype(BF16)
        for m in range(micro):
            row = ref[m : m + 1, :]
            hot = hot_of(row)
            before = jnp.dot(hot.astype(BF16), ahead, preferred_element_type=F32)
            slot = jnp.sum(hot * before, axis=0, keepdims=True) + row.astype(F32) * cap
            slot_row[side, m] = jnp.broadcast_to(slot, (8, tok))

    def assign_back(side):
        lanes = lax.broadcasted_iota(jnp.int32, (tok, slots_all), 1).astype(F32)
        for m in range(micro):
            slot = spread(slot_row[side, m, 0:1, :])
            wide = jnp.concatenate([slot] * (slots_all // tok), axis=1)
            back_hot[side, m] = jnp.where(lanes == wide, 1.0, 0.0).astype(BF16)

    def x_copy(side, to):
        return remote(
            xs.at[side, to], xr.at[side, e], x_sem.at[0, side], x_sem.at[1, side], expert=to
        )

    def x_keep(side):
        return pltpu.make_async_copy(xs.at[side, e], xr.at[side, e], x_own.at[side])

    def dispatch(side, tok_ref):
        for m in range(micro):
            hot = lax.broadcasted_iota(jnp.int32, (slots_all, tok), 0).astype(F32)
            hot = jnp.where(hot == slot_row[side, m, 0:1, :], 1.0, 0.0).astype(BF16)
            put = jnp.dot(hot, tok_ref[m], preferred_element_type=F32).astype(BF16)
            for to in range(experts):
                xs[side, to, m] = put[to * cap : (to + 1) * cap]
        for k in range(1, experts):
            x_copy(side, (e + k) % experts).start()
        x_keep(side).start()

    def x_landed(side):
        arrive(xr.at[side, pl.ds(1, experts - 1)], x_sem.at[1, side])
        x_keep(side).wait()

    assign(0, routes_ref)
    dispatch(0, tokens_ref)

    counted = jnp.zeros((8, experts), F32)
    summed = jnp.zeros((8, experts), F32)
    present = jnp.zeros((8, 1), F32)
    for m in range(micro):
        logits = lax.dot_general(
            router_ref[...], tokens_ref[m], (((1,), (1,)), ((), ())), preferred_element_type=F32
        )
        row = routes_ref[m : m + 1, :]
        hot = jnp.where(lax.broadcasted_iota(jnp.int32, (experts, tok), 0) == row, 1.0, 0.0)
        chosen = jnp.sum(logits * hot, axis=0, keepdims=True)
        gate[m] = spread(1.0 / (1.0 + jnp.exp(-chosen)))
        exps = jnp.exp(logits)
        probs = exps / jnp.sum(exps, axis=0, keepdims=True)
        modal = lax.broadcasted_iota(jnp.int32, (8, tok), 0) == modality_ref[m : m + 1, :]
        modal = jnp.where(modal, 1.0, 0.0)
        counted += lax.dot_general(
            modal, hot, (((1,), (1,)), ((), ())),
            precision=lax.Precision.HIGHEST, preferred_element_type=F32,
        )
        summed += lax.dot_general(
            modal, probs, (((1,), (1,)), ((), ())),
            precision=lax.Precision.HIGHEST, preferred_element_type=F32,
        )
        present += jnp.sum(modal, axis=1, keepdims=True)
    sums[0] = jnp.zeros((8, 128), F32)
    sums[0, 0:2, 0:experts] = counted[0:2]
    sums[0, 2:4, 0:experts] = summed[0:2]
    sums[0, 4:6, 0:experts] = jnp.broadcast_to(present[0:2], (2, experts))

    def tell_e(k, carry):
        remote(
            sums.at[0], stats_e.at[e], stat_sem.at[0, 0], stat_sem.at[1, 0], expert=(e + k) % experts
        ).start()
        return carry

    def tell_d(k, carry):
        remote(
            sums.at[1], stats_d.at[p], stat_sem.at[0, 1], stat_sem.at[1, 1], dp=(p + k) % ranks
        ).start()
        return carry

    lax.fori_loop(1, experts, tell_e, 0)
    assign_back(0)

    def second_stats():
        arrive(stats_e.at[pl.ds(1, experts - 1)], stat_sem.at[1, 0])
        stats_e[e] = sums[0]
        sums[1] = jnp.sum(stats_e[...], axis=0)
        lax.fori_loop(1, ranks, tell_d, 0)

    tile = 512 if half_ff % 512 == 0 else 128
    half_w = width // 2

    def first_dot(side, which, at):
        left = xr[side, :, :, :, pl.ds(pl.multiple_of(which * half_w, 128), half_w)]
        right = win[pl.ds(pl.multiple_of(which * half_w, 16), half_w), pl.ds(at, tile)]
        return jnp.dot(left.reshape(side_rows, half_w), right, preferred_element_type=F32)

    def near_side(side):
        def near_tile(i, carry):
            at = pl.multiple_of(i * tile, 128)
            acc[side, :, pl.ds(at, tile)] = first_dot(side, h, at)
            return carry

        lax.fori_loop(0, half_ff // tile, near_tile, 0)

    def far_sides(sides, j):
        start, size = splits[j]
        count = size // tile

        def far_tile(i, carry):
            side = i % sides
            at = pl.multiple_of(start + (i // sides) * tile, 128)
            pre = acc[side, :, pl.ds(at, tile)] + first_dot(side, 1 - h, at)
            hid[side, :, pl.ds(at, tile)] = jax.nn.gelu(pre, approximate=True).astype(BF16)
            return carry

        lax.fori_loop(0, count * sides, far_tile, 0)

    def near_arrived():
        for k in range(1, group):
            arrive(win_rows(peer(k)), in_recv.at[peer(k), 0])
            pass_near(k).start()

    def near_whole():
        own_in.wait()
        for k in range(group):
            q = (h * group + (zl + k) % group) * 2 + (1 - c)
            arrive(win_rows(q), in_recv.at[q, 0])

    def far_arrived(t, which, j):
        q = far_rank(t, which, c)
        arrive(win_rows(q, *splits[j]), in_recv.at[q, j])
        pass_far(q, j, 0).start()

    def far_direct(which, j):
        q = far_rank(0, which, c)
        arrive(win_rows(q, *splits[j]), in_recv.at[q, j])
        for k in range(1, group):
            pass_far(q, j, k).start()
        pass_far(q, j, 0).start()

    def far_whole(j):
        for t in range(pairs):
            for which in range(2):
                q = far_rank(t, which, 1 - c)
                arrive(win_rows(q, *splits[j]), in_recv.at[q, j])

    def out_arrived(i):
        for k in range(1, group):
            r = place(k, c)
            arrive(wout_rows(r, i), out_recv.at[r, i])
            pass_out(k, i).start()

    def out_whole(i):
        own_out[i].wait()
        for k in range(group):
            r = place(k, 1 - c)
            arrive(wout_rows(r, i), out_recv.at[r, i])

    def second(side, i):
        got = jnp.dot(
            hid[side], wout[:, i * tile_w : (i + 1) * tile_w], preferred_element_type=F32
        ).astype(BF16)
        ys[side, i] = got.reshape(experts, micro, cap, tile_w)

    def y_keep(side, i):
        return pltpu.make_async_copy(ys.at[side, i, e], yr.at[side, i, e], y_own.at[side, i])

    def y_start(side, i):
        for k in range(1, experts):
            to = (e + k) % experts
            remote(
                ys.at[side, i, to], yr.at[side, i, e], y_sem.at[0, side, i], y_sem.at[1, side, i],
                expert=to,
            ).start()
        y_keep(side, i).start()

    def y_landed(side, i):
        arrive(yr.at[side, i, pl.ds(1, experts - 1)], y_sem.at[1, side, i])
        y_keep(side, i).wait()

    def combine(side, i, m):
        back = yr[side, i, :, m].reshape(slots_all, tile_w)
        return jnp.dot(back_hot[side, m], back, preferred_element_type=F32)

    def z_copy(side, i):
        return remote(
            zs.at[side - 1, i], zr.at[i], z_send.at[side - 1, i], z_recv.at[i],
            dp=far_out if side == 1 else far_in,
        )

    def give_back(side, i):
        y_landed(side, i)
        for m in range(micro):
            zs[side - 1, i, m] = combine(side, i, m).astype(BF16)
        z_copy(side, i).start()

    last = len(splits) - 1

    @pl.when(inner)
    def _():
        for which in range(2):
            arrive(routes_far.at[which], routes_sem.at[1, which])
            arrive(tok_far.at[which], tok_sem.at[1, which])
            assign(1 + which, routes_far.at[which])
            dispatch(1 + which, tok_far.at[which])
            assign_back(1 + which)
        second_stats()
        near_arrived()
        x_landed(0)
        near_whole()
        near_side(0)
        x_landed(1)
        near_side(1)
        x_landed(2)
        near_side(2)
        for j in range(last + 1):
            far_direct(0, j)
        for copy in out_peers[early]:
            copy.start()
        for j in range(last + 1):
            far_direct(1, j)
            for t in range(1, pairs):
                far_arrived(t, 0, j)
                far_arrived(t, 1, j)
            if j == last:
                for i in range(early + 1, pieces):
                    for copy in out_peers[i]:
                        copy.start()
                out_arrived(0)
            far_whole(j)
            far_sides(3, j)
        for i in range(pieces):
            if i + 1 < pieces:
                out_arrived(i + 1)
            out_whole(i)
            for side in (2, 1):
                second(side, i)
                y_start(side, i)
            second(0, i)
            if i > 0:
                for side in (2, 1):
                    give_back(side, i - 1)
        for i in range(pieces):
            y_start(0, i)
        for side in (2, 1):
            give_back(side, pieces - 1)

    @pl.when(outer)
    def _():
        second_stats()
        near_arrived()
        x_landed(0)
        near_whole()
        near_side(0)
        for i in range(early):
            out_arrived(i)
        for j in range(last + 1):
            for t in range(pairs):
                far_arrived(t, 0, j)
                far_arrived(t, 1, j)
            far_whole(j)
            far_sides(1, j)
        for i in range(pieces):
            if i >= early:
                out_arrived(i)
            out_whole(i)
            second(0, i)
            y_start(0, i)

    arrive(stats_d.at[pl.ds(1, ranks - 1)], stat_sem.at[1, 1])
    stats_d[p] = sums[1]
    sums[2] = jnp.sum(stats_d[...], axis=0)
    modal_counts = sums[2, 4:6, 0:experts]
    load_ref[0] = experts * sums[2, 0:2, 0:experts] / modal_counts
    load_ref[1] = experts * sums[2, 2:4, 0:experts] / modal_counts

    for i in range(pieces):
        y_landed(0, i)
        kept = [combine(0, i, m) for m in range(micro)]
        arrive(zr.at[i], z_recv.at[i])
        for m in range(micro):
            both = kept[m] + zr[i, m].astype(F32)
            scale = jnp.concatenate([gate[m]] * (tile_w // tok), axis=1)
            mixed_ref[m, :, i * tile_w : (i + 1) * tile_w] = (both * scale).astype(BF16)

    arrive(stats_e.at[pl.ds(1, experts - 1)], stat_sem.at[0, 0])
    arrive(stats_d.at[pl.ds(1, ranks - 1)], stat_sem.at[0, 1])
    for copy in [tok_copy, routes_copy, near_mate] + far_copies + near_peers + out_mate:
        copy.wait_send()
    for i in range(pieces):
        for copy in out_peers[i]:
            copy.wait_send()
        for k in range(1, group):
            pass_out(k, i).wait_send()
    for k in range(1, group):
        pass_near(k).wait_send()
    for t in range(pairs):
        for which in range(2):
            for j in range(last + 1):
                pass_far(far_rank(t, which, c), j, 0).wait_send()

    def sent(side):
        arrive(xr.at[side, pl.ds(1, experts - 1)], x_sem.at[0, side])
        for i in range(pieces):
            arrive(yr.at[side, i, pl.ds(1, experts - 1)], y_sem.at[0, side, i])

    sent(0)

    @pl.when(inner)
    def _():
        for side in (1, 2):
            sent(side)
            for i in range(pieces):
                z_copy(side, i).wait_send()
        for which in range(2):
            for j in range(last + 1):
                for k in range(1, group):
                    pass_far(far_rank(0, which, c), j, k).wait_send()


def on_device(tokens, modality, routes, router, w_in, w_out):
    micro, tok, width = tokens.shape
    experts = router.shape[1]
    cap = 2 * tok // experts
    ranks = lax.axis_size("dp")
    group = ranks // 4
    half_ff = w_in.shape[2] // 2
    tile_w = 256 if width % 256 == 0 else 128
    pieces = width // tile_w
    tile = 512 if half_ff % 512 == 0 else 128
    first = (half_ff // tile + 1) // 2 * tile
    splits = ((0, first), (first, half_ff - first))
    parts = len(splits)

    dma = pltpu.SemaphoreType.DMA
    vmem = pl.BlockSpec(memory_space=pltpu.VMEM)
    hbm = pl.BlockSpec(memory_space=pl.ANY)
    rows = experts * micro * cap
    mixed, load = pl.pallas_call(
        functools.partial(layer_kernel, experts, ranks, splits),
        out_shape=(
            jax.ShapeDtypeStruct(tokens.shape, BF16),
            jax.ShapeDtypeStruct((2, 2, experts), F32),
        ),
        in_specs=[vmem] * 4 + [hbm] * 2,
        out_specs=(vmem, vmem),
        scratch_shapes=[
            pltpu.VMEM((2, micro, tok, width), BF16),
            pltpu.VMEM((2, micro, tok), jnp.int32),
            pltpu.VMEM((3, micro, 8, tok), F32),
            pltpu.VMEM((3, micro, tok, experts * cap), BF16),
            pltpu.VMEM((micro, tok, tok), F32),
            pltpu.VMEM((3, 8, 128), F32),
            pltpu.VMEM((experts, 8, 128), F32),
            pltpu.VMEM((ranks, 8, 128), F32),
            pltpu.VMEM((width, half_ff), BF16),
            pltpu.VMEM((half_ff, width), BF16),
            pltpu.VMEM((3, experts, micro, cap, width), BF16),
            pltpu.VMEM((3, experts, micro, cap, width), BF16),
            pltpu.VMEM((3, rows, half_ff), F32),
            pltpu.VMEM((3, rows, half_ff), BF16),
            pltpu.VMEM((3, pieces, experts, micro, cap, tile_w), BF16),
            pltpu.VMEM((3, pieces, experts, micro, cap, tile_w), BF16),
            pltpu.VMEM((2, pieces, micro, tok, tile_w), BF16),
            pltpu.VMEM((pieces, micro, tok, tile_w), BF16),
            dma((2, 2)),
            dma((2, 2)),
            dma((2, 2)),
            dma((parts,)),
            dma((ranks, parts, group)),
            dma((ranks, parts)),
            dma((2 * group, pieces, group)),
            dma((2 * group, pieces)),
            dma((2, 3)),
            dma((3,)),
            dma((2, 3, pieces)),
            dma((3, pieces)),
            dma((2, pieces)),
            dma((pieces,)),
        ],
        compiler_params=pltpu.CompilerParams(
            collective_id=0, has_side_effects=True, vmem_limit_bytes=64 * 1024 * 1024 - 65536
        ),
    )(tokens, routes[:, :, 0], modality, router.T, w_in[0], w_out[0])
    return (mixed, load)


def solution(mesh):
    placed = (
        P(None, ("expert", "dp"), None),
        P(None, ("expert", "dp")),
        P(None, ("expert", "dp"), None),
        P(),
        P("expert", "dp", None),
        P("expert", "dp", None),
    )
    return jax.shard_map(
        on_device,
        mesh=mesh,
        in_specs=placed,
        out_specs=(P(None, ("expert", "dp"), None), P()),
        check_vma=False,
    )
```

```python
import functools
import math

import jax
import jax.numpy as jnp
from jax import lax
from jax.experimental import pallas as pl
from jax.experimental.pallas import tpu as pltpu
from jax.sharding import PartitionSpec as P

MESH = pl.DeviceIdType.MESH
BF16 = jnp.bfloat16
F32 = jnp.float32
C1 = math.sqrt(2 / math.pi)
C3 = 0.044715 * C1


def layer_kernel(
    experts,
    ranks,
    tile,
    tokens_ref,
    routes_ref,
    modality_ref,
    router_ref,
    w_in_ref,
    w_out_ref,
    mixed_ref,
    load_ref,
    tok_own,
    result,
    tok_far,
    routes_far,
    slot_row,
    back_hot,
    gate,
    sums,
    stats_e,
    stats_d,
    win,
    wout,
    xs,
    xr,
    acc,
    hid,
    ys,
    yr,
    zs,
    zr,
    w_part,
    tok_sem,
    routes_sem,
    stat_sem,
    in_send,
    near_recv,
    near_whole_recv,
    far_recv,
    far_whole_recv,
    out_send,
    out_recv,
    out_whole_recv,
    x_sem,
    y_send,
    y_recv,
    z_send,
    z_recv,
    w_send,
    w_recv,
    load_sem,
    result_sem,
):
    micro, tok, width = tokens_ref.shape
    in_rows, ff = w_in_ref.shape
    out_rows = w_out_ref.shape[0]
    half_ff = ff // 2
    pieces, tile_w = zr.shape[0], zr.shape[3]
    direct = w_part.shape[0]
    cap = xs.shape[3]
    slots_all = experts * cap
    side_rows = experts * micro * cap
    e = lax.axis_index("expert")
    p = lax.axis_index("dp")
    z, c = p // 2, p % 2
    chips = ranks // 2
    group = chips // 2
    pairs = group // 2
    h = z // group
    zl = z % group
    mate = z * 2 + (1 - c)
    inner = (z % 2) == (1 - h)
    outer = (z % 2) == h
    role = (z + h) % 2

    def far_rank(t, which, core):
        pair = (1 - h) * pairs + ((z // 2) % pairs + t) % pairs
        return (pair * 2 + (1 - h + which) % 2) * 2 + core

    far_in = far_rank(0, 1, c)
    far_out = far_rank(0, 0, c)

    def peer(k):
        return (h * group + (zl + k) % group) * 2 + c

    def place(k, core):
        return ((zl + k) % group) * 2 + core

    tok_load = pltpu.make_async_copy(tokens_ref, tok_own, load_sem)
    tok_load.start()
    barrier = pltpu.get_barrier_semaphore()

    def greet_e(k, carry):
        pl.semaphore_signal(
            barrier, inc=1, device_id=((e + k) % experts, p), device_id_type=MESH
        )
        return carry

    def greet_d(k, carry):
        pl.semaphore_signal(barrier, inc=1, device_id=(e, (p + k) % ranks), device_id_type=MESH)
        return carry

    lax.fori_loop(1, experts, greet_e, 0)
    lax.fori_loop(1, ranks, greet_d, 0)

    def remote(src, dst, send, recv, dp=None, expert=None):
        return pltpu.make_async_remote_copy(
            src_ref=src,
            dst_ref=dst,
            send_sem=send,
            recv_sem=recv,
            device_id=(e if expert is None else expert, p if dp is None else dp),
            device_id_type=MESH,
        )

    def arrive(ref, sem):
        pltpu.make_async_copy(ref, ref, sem).wait()

    parts = half_ff // tile

    def chunk(j):
        return (j * tile if isinstance(j, int) else pl.multiple_of(j * tile, 128), tile)

    def win_rows(q, start=0, size=half_ff):
        return win.at[pl.ds(pl.multiple_of(q * in_rows, 16), in_rows), pl.ds(start, size)]

    def wout_rows(r, piece):
        return wout.at[
            pl.ds(pl.multiple_of(r * out_rows, 16), out_rows), pl.ds(piece * tile_w, tile_w)
        ]

    def cols(which, start=0, size=half_ff):
        return w_in_ref.at[:, pl.ds(pl.multiple_of(which * half_ff + start, 128), size)]

    def w_out_piece(piece):
        return w_out_ref.at[:, pl.ds(piece * tile_w, tile_w)]

    tok_copy = remote(
        tok_own, tok_far.at[role], tok_sem.at[2], tok_sem.at[role], dp=far_in
    )
    routes_copy = remote(
        routes_ref, routes_far.at[role], routes_sem.at[2], routes_sem.at[role], dp=far_in
    )
    far_copies = [
        remote(
            cols(1 - h, *chunk(j)), win_rows(p, *chunk(j)), in_send.at[0], far_recv.at[zl, j], dp=far_in
        )
        for j in range(parts)
    ]
    near_peers = [
        remote(cols(h), win_rows(p), in_send.at[0], near_recv.at[zl], dp=peer(k))
        for k in range(1, group)
    ]
    near_mate = remote(cols(h), win_rows(p), in_send.at[0], near_whole_recv, dp=mate)
    own_in = pltpu.make_async_copy(cols(h), win_rows(p), near_whole_recv)
    mine = place(0, c)
    out_peers = [
        [
            remote(
                w_out_piece(i), wout_rows(mine, i), out_send, out_recv.at[zl, i], dp=peer(k)
            )
            for k in range(1, group)
        ]
        for i in range(pieces)
    ]
    out_mate = [
        remote(
            w_out_piece(i), wout_rows(mine, i), out_send, out_whole_recv.at[i], dp=mate
        )
        for i in range(pieces)
    ]
    own_out = [
        pltpu.make_async_copy(w_out_piece(i), wout_rows(mine, i), out_whole_recv.at[i])
        for i in range(pieces)
    ]

    def pass_near(k):
        q = peer(k)
        return remote(win_rows(q), win_rows(q), in_send.at[0], near_whole_recv, dp=mate)

    def pass_far(q, j, k):
        rows = win_rows(q, *chunk(j))
        if k == 0:
            return remote(rows, rows, in_send.at[0], far_whole_recv.at[j], dp=mate)
        at = (q // 2) % group
        return remote(rows, rows, in_send.at[1], far_recv.at[at, j], dp=peer(k))

    def pass_out(k, i):
        r = place(k, c)
        rows = wout_rows(r, i)
        return remote(rows, rows, out_send, out_whole_recv.at[i], dp=mate)

    tok_load.wait()
    pl.semaphore_wait(barrier, experts + ranks - 2)

    early = pieces - 1
    routes_copy.start()
    tok_copy.start()

    @pl.when(inner)
    def _():
        for copy in far_copies:
            copy.start()
        for copy in near_peers:
            copy.start()
        for i in range(2):
            for copy in out_peers[i]:
                copy.start()

    @pl.when(outer)
    def _():
        for copy in far_copies[:2]:
            copy.start()
        for copy in near_peers:
            copy.start()
        for copy in far_copies[2:]:
            copy.start()
        for i in range(pieces):
            for copy in out_peers[i]:
                copy.start()


    rows_e = max(experts, 8)

    def hot_of(row):
        at = lax.broadcasted_iota(jnp.int32, (rows_e, tok), 0)
        return jnp.where(at == row, 1.0, 0.0)

    def spread(row):
        return jnp.broadcast_to(row, (tok, tok)).T

    def assign(side, ref):
        ahead = lax.broadcasted_iota(jnp.int32, (tok, tok), 0) < lax.broadcasted_iota(
            jnp.int32, (tok, tok), 1
        )
        ahead = jnp.where(ahead, 1.0, 0.0).astype(BF16)
        for m in range(micro):
            row = ref[m : m + 1, :]
            hot = hot_of(row)
            before = jnp.dot(hot.astype(BF16), ahead, preferred_element_type=F32)
            slot = jnp.sum(hot * before, axis=0, keepdims=True) + row.astype(F32) * cap
            slot_row[side, m] = jnp.broadcast_to(slot, (8, tok))

    def assign_back(side):
        lanes = lax.broadcasted_iota(jnp.int32, (tok, slots_all), 1).astype(F32)
        for m in range(micro):
            slot = spread(slot_row[side, m, 0:1, :])
            wide = jnp.concatenate([slot] * (slots_all // tok), axis=1)
            back_hot[side, m] = jnp.where(lanes == wide, 1.0, 0.0).astype(BF16)

    def x_copy(side, to):
        return remote(
            xs.at[side, to], xr.at[side, e], x_sem.at[0, side], x_sem.at[1, side], expert=to
        )

    def dispatch(side, tok_ref):
        for m in range(micro):
            hot = lax.broadcasted_iota(jnp.int32, (slots_all, tok), 0).astype(F32)
            hot = jnp.where(hot == slot_row[side, m, 0:1, :], 1.0, 0.0).astype(BF16)
            put = jnp.dot(hot, tok_ref[m], preferred_element_type=F32).astype(BF16)
            for to in range(experts):
                xs[side, to, m] = put[to * cap : (to + 1) * cap]
        for k in range(1, experts):
            x_copy(side, (e + k) % experts).start()
        xr[side, e] = xs[side, e]

    def x_landed(side):
        arrive(xr.at[side, pl.ds(1, experts - 1)], x_sem.at[1, side])

    assign(0, routes_ref)
    dispatch(0, tok_own)
    near_mate.start()
    own_in.start()

    counted = jnp.zeros((8, experts), F32)
    summed = jnp.zeros((8, experts), F32)
    present = jnp.zeros((8, 1), F32)
    for m in range(micro):
        logits = lax.dot_general(
            router_ref[...], tok_own[m], (((1,), (1,)), ((), ())), preferred_element_type=F32
        )
        row = routes_ref[m : m + 1, :]
        hot = jnp.where(lax.broadcasted_iota(jnp.int32, (experts, tok), 0) == row, 1.0, 0.0)
        chosen = jnp.sum(logits * hot, axis=0, keepdims=True)
        gate[m] = spread(1.0 / (1.0 + jnp.exp(-chosen)))
        exps = jnp.exp(logits)
        probs = exps / jnp.sum(exps, axis=0, keepdims=True)
        modal = lax.broadcasted_iota(jnp.int32, (8, tok), 0) == modality_ref[m : m + 1, :]
        modal = jnp.where(modal, 1.0, 0.0)
        counted += lax.dot_general(
            modal, hot, (((1,), (1,)), ((), ())),
            precision=lax.Precision.HIGHEST, preferred_element_type=F32,
        )
        summed += lax.dot_general(
            modal, probs, (((1,), (1,)), ((), ())),
            precision=lax.Precision.HIGHEST, preferred_element_type=F32,
        )
        present += jnp.sum(modal, axis=1, keepdims=True)
    sums[0] = jnp.zeros((8, 128), F32)
    sums[0, 0:2, 0:experts] = counted[0:2]
    sums[0, 2:4, 0:experts] = summed[0:2]
    sums[0, 4:6, 0:experts] = jnp.broadcast_to(present[0:2], (2, experts))

    def tell_e(k, carry):
        remote(
            sums.at[0], stats_e.at[e], stat_sem.at[0, 0], stat_sem.at[1, 0], expert=(e + k) % experts
        ).start()
        return carry

    def tell_d(k, carry):
        remote(
            sums.at[1], stats_d.at[p], stat_sem.at[0, 1], stat_sem.at[1, 1], dp=(p + k) % ranks
        ).start()
        return carry

    lax.fori_loop(1, experts, tell_e, 0)
    for i in range(pieces):
        out_mate[i].start()
        own_out[i].start()
    assign_back(0)

    def second_stats():
        arrive(stats_e.at[pl.ds(1, experts - 1)], stat_sem.at[1, 0])
        stats_e[e] = sums[0]
        sums[1] = jnp.sum(stats_e[...], axis=0)
        lax.fori_loop(1, ranks, tell_d, 0)

    half_w = width // 2

    def first_dot(side, which, at):
        left = xr[side, :, :, :, pl.ds(pl.multiple_of(which * half_w, 128), half_w)]
        right = win[pl.ds(pl.multiple_of(which * half_w, 16), half_w), pl.ds(at, tile)]
        return jnp.dot(left.reshape(side_rows, half_w), right, preferred_element_type=F32)

    def near_side(side):
        def near_tile(i, carry):
            at = pl.multiple_of(i * tile, 128)
            acc[side, :, pl.ds(at, tile)] = first_dot(side, h, at)
            return carry

        lax.fori_loop(0, half_ff // tile, near_tile, 0)

    def far_sides(sides, j):
        at = pl.multiple_of(j * tile, 128)
        for side in range(sides):
            pre = acc[side, :, pl.ds(at, tile)] + first_dot(side, 1 - h, at)
            half = 0.5 * pre
            curve = jnp.tanh(pre * (C1 + C3 * (pre * pre)))
            hid[side, :, pl.ds(at, tile)] = (half + half * curve).astype(BF16)

    def win_span(blocks, at=0, size=half_ff):
        return win.at[pl.ds(0, blocks * in_rows), pl.ds(at, size)]

    def near_arrived():
        for k in range(1, group):
            arrive(win_rows(peer(k)), near_recv.at[(zl + k) % group])
            pass_near(k).start()

    def near_whole():
        arrive(win_span(group + 1), near_whole_recv)

    def far_arrived(t, which, j):
        q = far_rank(t, which, c)
        arrive(win_rows(q, *chunk(j)), far_recv.at[(q // 2) % group, j])
        pass_far(q, j, 0).start()

    def far_direct(which, j):
        q = far_rank(0, which, c)
        arrive(win_rows(q, *chunk(j)), far_recv.at[(q // 2) % group, j])
        for k in range(1, group):
            pass_far(q, j, k).start()
        pass_far(q, j, 0).start()

    def far_whole(j):
        arrive(win_span(group, *chunk(j)), far_whole_recv.at[j])

    def out_arrived(i):
        for k in range(1, group):
            arrive(wout_rows(place(k, c), i), out_recv.at[(zl + k) % group, i])
            pass_out(k, i).start()

    def out_whole(i):
        span = wout.at[pl.ds(0, (group + 1) * out_rows), pl.ds(i * tile_w, tile_w)]
        arrive(span, out_whole_recv.at[i])

    block = side_rows // 2
    block_e = experts // 2

    def second(i, low, high):
        def step(k, carry):
            side, at = low + k // 2, pl.multiple_of((k % 2) * block, 16)
            got = jnp.dot(
                hid[side, pl.ds(at, block), :],
                wout[:, i * tile_w : (i + 1) * tile_w],
                preferred_element_type=F32,
            )
            if i < direct and low == 0:
                near = w_part[i, pl.ds((k % 2) * block_e, block_e)].reshape(block, tile_w)
                got += jnp.where(inner, near.astype(F32), 0.0)
            got = got.astype(BF16).reshape(block_e, micro, cap, tile_w)
            ys[side, i, pl.ds((k % 2) * block_e, block_e)] = got
            return carry

        lax.fori_loop(0, 2 * (high - low), step, 0)

    def w_copy(i):
        return remote(ys.at[2, i], w_part.at[i], w_send, w_recv.at[i], dp=far_in)

    def y_start(side, i):
        for k in range(1, experts):
            to = (e + k) % experts
            remote(
                ys.at[side, i, to], yr.at[side, i, e], y_send.at[side], y_recv.at[side, i], expert=to
            ).start()
        yr[side, i, e] = ys[side, i, e]

    def y_landed(side, i):
        arrive(yr.at[side, i, pl.ds(1, experts - 1)], y_recv.at[side, i])

    def combine(side, i, m):
        back = yr[side, i, :, m].reshape(slots_all, tile_w)
        return jnp.dot(back_hot[side, m], back, preferred_element_type=F32)

    def z_copy(side, i):
        return remote(
            zs.at[side - 1, i], zr.at[i], z_send.at[side - 1], z_recv.at[i],
            dp=far_out if side == 1 else far_in,
        )

    def give_back(side, i):
        y_landed(side, i)
        for m in range(micro):
            zs[side - 1, i, m] = combine(side, i, m).astype(BF16)
        z_copy(side, i).start()

    @pl.when(inner)
    def _():
        for which in range(2):
            arrive(routes_far.at[which], routes_sem.at[which])
            arrive(tok_far.at[which], tok_sem.at[which])
            assign(1 + which, routes_far.at[which])
            dispatch(1 + which, tok_far.at[which])
            assign_back(1 + which)
            if which == 0:
                far_direct(0, 0)
                far_direct(0, 1)
                for i in range(2, early):
                    for copy in out_peers[i]:
                        copy.start()
        second_stats()
        near_arrived()
        x_landed(0)
        near_whole()
        near_side(0)
        x_landed(1)
        near_side(1)
        x_landed(2)
        near_side(2)
        for j in range(2, parts):
            far_direct(0, j)

        def far_next(j):
            far_direct(1, j)
            for t in range(1, pairs):
                far_arrived(t, 0, j)
                far_arrived(t, 1, j)

        far_next(0)

        def far_step(j, carry):
            @pl.when(j < parts - 1)
            def _():
                far_next(j + 1)

            @pl.when(j == parts - 2)
            def _():
                for i in range(early, pieces):
                    for copy in out_peers[i]:
                        copy.start()
                out_arrived(0)

            far_whole(j)
            far_sides(3, j)
            return carry

        lax.fori_loop(0, parts, far_step, 0)

        def own(i):
            if i < direct:
                arrive(w_part.at[i], w_recv.at[i])
            second(i, 0, 1)

        def far_piece(i):
            out_whole(i)
            second(i, 1, 2)
            y_start(1, i)
            second(i, 2, 3)
            if i < direct:
                w_copy(i).start()
            else:
                y_start(2, i)

        out_arrived(1)
        far_piece(0)
        far_piece(1)
        for i in range(2, pieces):
            if i >= pieces - 2:
                give_back(1, i - pieces + 2)
            out_arrived(i)
            if i == pieces - 2:
                own(0)
                y_start(0, 0)
            if i == pieces - 1:
                own(1)
            far_piece(i)
            if i == pieces - 2:
                give_back(2, i - 1)
        y_start(0, 1)
        for i in range(2, pieces):
            own(i)
            y_start(0, i)
        give_back(2, pieces - 2)
        for i in range(2, pieces):
            give_back(1, i)
        give_back(2, pieces - 1)

    @pl.when(outer)
    def _():
        second_stats()
        near_arrived()
        x_landed(0)
        near_whole()
        near_side(0)
        for i in range(early):
            out_arrived(i)

        def far_step(j, carry):
            for t in range(pairs):
                far_arrived(t, 0, j)
                far_arrived(t, 1, j)
            far_whole(j)
            far_sides(1, j)
            return carry

        lax.fori_loop(0, parts, far_step, 0)
        for i in range(pieces):
            if i >= early:
                out_arrived(i)
            out_whole(i)
            second(i, 0, 1)
            y_start(0, i)

    arrive(stats_d.at[pl.ds(1, ranks - 1)], stat_sem.at[1, 1])
    stats_d[p] = sums[1]
    sums[2] = jnp.sum(stats_d[...], axis=0)
    modal_counts = sums[2, 4:6, 0:experts]
    load_ref[0] = experts * sums[2, 0:2, 0:experts] / modal_counts
    load_ref[1] = experts * sums[2, 2:4, 0:experts] / modal_counts

    @pl.when(inner)
    def _():
        for i in range(direct):
            zr[i] = jnp.zeros((micro, tok, tile_w), BF16)

    def result_copy(i):
        part = (slice(None), slice(None), pl.ds(i * tile_w, tile_w))
        return pltpu.make_async_copy(result.at[part], mixed_ref.at[part], result_sem)

    arrive(stats_e.at[pl.ds(1, experts - 1)], stat_sem.at[0, 0])
    arrive(stats_d.at[pl.ds(1, ranks - 1)], stat_sem.at[0, 1])
    tok_copy.wait_send()
    routes_copy.wait_send()
    arrive(win_span(3 * group), in_send.at[0])
    arrive(wout.at[pl.ds(0, (2 * group - 1) * out_rows), :], out_send)
    arrive(xr.at[0, pl.ds(1, experts - 1)], x_sem.at[0, 0])

    @pl.when(inner)
    def _():
        arrive(win_span(2 * (group - 1)), in_send.at[1])
        for side in (1, 2):
            arrive(xr.at[side, pl.ds(1, experts - 1)], x_sem.at[0, side])
        arrive(yr.at[1, :, pl.ds(1, experts - 1)], y_send.at[1])
        arrive(yr.at[2, pl.ds(direct, pieces - direct), pl.ds(1, experts - 1)], y_send.at[2])
        arrive(w_part, w_send)

    for i in range(pieces):
        y_landed(0, i)
        kept = [combine(0, i, m) for m in range(micro)]
        if i < direct:

            @pl.when(outer)
            def _(i=i):
                arrive(zr.at[i], z_recv.at[i])
        else:
            arrive(zr.at[i], z_recv.at[i])
        for m in range(micro):
            both = kept[m] + zr[i, m].astype(F32)
            scale = jnp.concatenate([gate[m]] * (tile_w // tok), axis=1)
            result[m, :, i * tile_w : (i + 1) * tile_w] = (both * scale).astype(BF16)
        result_copy(i).start()

    arrive(yr.at[0, :, pl.ds(1, experts - 1)], y_send.at[0])
    pltpu.make_async_copy(result, mixed_ref, result_sem).wait()

    @pl.when(inner)
    def _():
        arrive(zs.at[0], z_send.at[0])
        arrive(zs.at[1, pl.ds(direct, pieces - direct)], z_send.at[1])


def on_device(tokens, modality, routes, router, w_in, w_out):
    micro, tok, width = tokens.shape
    experts = router.shape[1]
    cap = 2 * tok // experts
    ranks = lax.axis_size("dp")
    group = ranks // 4
    half_ff = w_in.shape[2] // 2
    tile_w = 256 if width % 256 == 0 else 128
    pieces = width // tile_w
    tile = 512 if half_ff % 512 == 0 else 128
    parts = half_ff // tile

    dma = pltpu.SemaphoreType.DMA
    vmem = pl.BlockSpec(memory_space=pltpu.VMEM)
    hbm = pl.BlockSpec(memory_space=pl.ANY)
    rows = experts * micro * cap
    mixed, load = pl.pallas_call(
        functools.partial(layer_kernel, experts, ranks, tile),
        out_shape=(
            jax.ShapeDtypeStruct(tokens.shape, BF16),
            jax.ShapeDtypeStruct((2, 2, experts), F32),
        ),
        in_specs=[hbm] + [vmem] * 3 + [hbm] * 2,
        out_specs=(hbm, vmem),
        scratch_shapes=[
            pltpu.VMEM((micro, tok, width), BF16),
            pltpu.VMEM((micro, tok, width), BF16),
            pltpu.VMEM((2, micro, tok, width), BF16),
            pltpu.VMEM((2, micro, tok), jnp.int32),
            pltpu.VMEM((3, micro, 8, tok), F32),
            pltpu.VMEM((3, micro, tok, experts * cap), BF16),
            pltpu.VMEM((micro, tok, tok), F32),
            pltpu.VMEM((3, 8, 128), F32),
            pltpu.VMEM((experts, 8, 128), F32),
            pltpu.VMEM((ranks, 8, 128), F32),
            pltpu.VMEM((width, half_ff), BF16),
            pltpu.VMEM((half_ff, width), BF16),
            pltpu.VMEM((3, experts, micro, cap, width), BF16),
            pltpu.VMEM((3, experts, micro, cap, width), BF16),
            pltpu.VMEM((3, rows, half_ff), F32),
            pltpu.VMEM((3, rows, half_ff), BF16),
            pltpu.VMEM((3, pieces, experts, micro, cap, tile_w), BF16),
            pltpu.VMEM((3, pieces, experts, micro, cap, tile_w), BF16),
            pltpu.VMEM((2, pieces, micro, tok, tile_w), BF16),
            pltpu.VMEM((pieces, micro, tok, tile_w), BF16),
            pltpu.VMEM((2, experts, micro, cap, tile_w), BF16),
            dma((3,)),
            dma((3,)),
            dma((2, 2)),
            dma((2,)),
            dma((group,)),
            dma,
            dma((group, parts)),
            dma((parts,)),
            dma,
            dma((group, pieces)),
            dma((pieces,)),
            dma((2, 3)),
            dma((3,)),
            dma((3, pieces)),
            dma((2,)),
            dma((pieces,)),
            dma,
            dma((2,)),
            dma,
            dma,
        ],
        compiler_params=pltpu.CompilerParams(
            collective_id=0, has_side_effects=True, vmem_limit_bytes=64 * 1024 * 1024 - 65536
        ),
    )(tokens, routes[:, :, 0], modality, router.T, w_in[0], w_out[0])
    return (mixed, load)


def solution(mesh):
    placed = (
        P(None, ("expert", "dp"), None),
        P(None, ("expert", "dp")),
        P(None, ("expert", "dp"), None),
        P(),
        P("expert", "dp", None),
        P("expert", "dp", None),
    )
    return jax.shard_map(
        on_device,
        mesh=mesh,
        in_specs=placed,
        out_specs=(P(None, ("expert", "dp"), None), P()),
        check_vma=False,
    )
```

```python
import functools
import math

import jax
import jax.numpy as jnp
from jax import lax
from jax.experimental import pallas as pl
from jax.experimental.pallas import tpu as pltpu
from jax.sharding import PartitionSpec as P

MESH = pl.DeviceIdType.MESH
BF16 = jnp.bfloat16
F32 = jnp.float32
C1 = math.sqrt(2 / math.pi)
C3 = 0.044715 * C1


def layer_kernel(
    experts,
    ranks,
    tile,
    far_tile,
    tokens_ref,
    routes_ref,
    modality_ref,
    router_ref,
    w_in_ref,
    w_out_ref,
    mixed_ref,
    load_ref,
    tok_own,
    tok_far,
    routes_far,
    slot_row,
    back_hot,
    gate,
    sums,
    stats_e,
    stats_d,
    win,
    wout,
    xs,
    xr,
    acc,
    hid,
    ys,
    yr,
    zs,
    zr,
    w_part,
    tok_sem,
    routes_sem,
    stat_sem,
    in_send,
    near_recv,
    near_whole_recv,
    far_recv,
    far_whole_recv,
    out_send,
    out_recv,
    out_whole_recv,
    x_sem,
    y_send,
    y_recv,
    z_send,
    z_recv,
    w_send,
    w_recv,
    load_sem,
):
    micro, tok, width = tokens_ref.shape
    in_rows, ff = w_in_ref.shape
    out_rows = w_out_ref.shape[0]
    half_ff = ff // 2
    pieces, tile_w = zr.shape[0], zr.shape[3]
    direct = w_part.shape[0]
    cap = xs.shape[3]
    slots_all = experts * cap
    side_rows = experts * micro * cap
    e = lax.axis_index("expert")
    p = lax.axis_index("dp")
    z, c = p // 2, p % 2
    chips = ranks // 2
    group = chips // 2
    pairs = group // 2
    h = z // group
    zl = z % group
    mate = z * 2 + (1 - c)
    inner = (z % 2) == (1 - h)
    outer = (z % 2) == h
    role = (z + h) % 2

    def far_rank(t, which, core):
        pair = (1 - h) * pairs + ((z // 2) % pairs + t) % pairs
        return (pair * 2 + (1 - h + which) % 2) * 2 + core

    far_in = far_rank(0, 1, c)
    far_out = far_rank(0, 0, c)

    def peer(k):
        return (h * group + (zl + k) % group) * 2 + c

    def place(k, core):
        return ((zl + k) % group) * 2 + core

    tok_load = pltpu.make_async_copy(tokens_ref, tok_own, load_sem)
    tok_load.start()
    barrier = pltpu.get_barrier_semaphore()

    def greet_e(k, carry):
        pl.semaphore_signal(
            barrier, inc=1, device_id=((e + k) % experts, p), device_id_type=MESH
        )
        return carry

    def greet_d(k, carry):
        pl.semaphore_signal(barrier, inc=1, device_id=(e, (p + k) % ranks), device_id_type=MESH)
        return carry

    lax.fori_loop(1, experts, greet_e, 0)
    lax.fori_loop(1, ranks, greet_d, 0)

    def remote(src, dst, send, recv, dp=None, expert=None):
        return pltpu.make_async_remote_copy(
            src_ref=src,
            dst_ref=dst,
            send_sem=send,
            recv_sem=recv,
            device_id=(e if expert is None else expert, p if dp is None else dp),
            device_id_type=MESH,
        )

    def arrive(ref, sem):
        pltpu.make_async_copy(ref, ref, sem).wait()

    parts = half_ff // far_tile
    ahead_parts = parts * 2 // 5

    def chunk(j):
        at = j * far_tile
        return (at if isinstance(j, int) else pl.multiple_of(at, 128), far_tile)

    def win_rows(q, start=0, size=half_ff):
        return win.at[pl.ds(pl.multiple_of(q * in_rows, 16), in_rows), pl.ds(start, size)]

    def wout_rows(r, piece):
        return wout.at[
            pl.ds(pl.multiple_of(r * out_rows, 16), out_rows), pl.ds(piece * tile_w, tile_w)
        ]

    def cols(which, start=0, size=half_ff):
        return w_in_ref.at[:, pl.ds(pl.multiple_of(which * half_ff + start, 128), size)]

    def w_out_piece(piece):
        return w_out_ref.at[:, pl.ds(piece * tile_w, tile_w)]

    tok_copy = remote(
        tok_own, tok_far.at[role], tok_sem.at[2], tok_sem.at[role], dp=far_in
    )
    routes_copy = remote(
        routes_ref, routes_far.at[role], routes_sem.at[2], routes_sem.at[role], dp=far_in
    )
    far_copies = [
        remote(
            cols(1 - h, *chunk(j)), win_rows(p, *chunk(j)), in_send.at[0], far_recv.at[zl, j], dp=far_in
        )
        for j in range(parts)
    ]
    near_peers = [
        remote(cols(h), win_rows(p), in_send.at[0], near_recv.at[zl], dp=peer(k))
        for k in range(1, group)
    ]
    near_mate = remote(cols(h), win_rows(p), in_send.at[0], near_whole_recv, dp=mate)
    own_in = pltpu.make_async_copy(cols(h), win_rows(p), near_whole_recv)
    mine = place(0, c)
    out_peers = [
        [
            remote(
                w_out_piece(i), wout_rows(mine, i), out_send, out_recv.at[zl, i], dp=peer(k)
            )
            for k in range(1, group)
        ]
        for i in range(pieces)
    ]
    out_mate = [
        remote(
            w_out_piece(i), wout_rows(mine, i), out_send, out_whole_recv.at[i], dp=mate
        )
        for i in range(pieces)
    ]
    own_out = [
        pltpu.make_async_copy(w_out_piece(i), wout_rows(mine, i), out_whole_recv.at[i])
        for i in range(pieces)
    ]

    def pass_near(k):
        q = peer(k)
        return remote(win_rows(q), win_rows(q), in_send.at[0], near_whole_recv, dp=mate)

    def pass_far(q, j, k):
        rows = win_rows(q, *chunk(j))
        if k == 0:
            return remote(rows, rows, in_send.at[0], far_whole_recv.at[j], dp=mate)
        at = (q // 2) % group
        return remote(rows, rows, in_send.at[1], far_recv.at[at, j], dp=peer(k))

    def pass_out(k, i):
        r = place(k, c)
        rows = wout_rows(r, i)
        return remote(rows, rows, out_send, out_whole_recv.at[i], dp=mate)

    tok_load.wait()
    pl.semaphore_wait(barrier, experts + ranks - 2)

    early = pieces - 2
    routes_copy.start()
    tok_copy.start()

    @pl.when(inner)
    def _():
        for copy in far_copies:
            copy.start()
        for copy in near_peers:
            copy.start()
        for i in range(2):
            for copy in out_peers[i]:
                copy.start()

    @pl.when(outer)
    def _():
        for copy in far_copies[:ahead_parts]:
            copy.start()
        for copy in near_peers:
            copy.start()
        for copy in far_copies[ahead_parts:]:
            copy.start()
        for i in range(pieces):
            for copy in out_peers[i]:
                copy.start()


    rows_e = max(experts, 8)

    def hot_of(row):
        at = lax.broadcasted_iota(jnp.int32, (rows_e, tok), 0)
        return jnp.where(at == row, 1.0, 0.0)

    def spread(row):
        return jnp.broadcast_to(row, (tok, tok)).T

    def assign(side, ref):
        ahead = lax.broadcasted_iota(jnp.int32, (tok, tok), 0) < lax.broadcasted_iota(
            jnp.int32, (tok, tok), 1
        )
        ahead = jnp.where(ahead, 1.0, 0.0).astype(BF16)
        for m in range(micro):
            row = ref[m : m + 1, :]
            hot = hot_of(row)
            before = jnp.dot(hot.astype(BF16), ahead, preferred_element_type=F32)
            slot = jnp.sum(hot * before, axis=0, keepdims=True) + row.astype(F32) * cap
            slot_row[side, m] = jnp.broadcast_to(slot, (8, tok))

    def assign_back(side):
        lanes = lax.broadcasted_iota(jnp.int32, (tok, slots_all), 1).astype(F32)
        for m in range(micro):
            slot = spread(slot_row[side, m, 0:1, :])
            wide = jnp.concatenate([slot] * (slots_all // tok), axis=1)
            back_hot[side, m] = jnp.where(lanes == wide, 1.0, 0.0).astype(BF16)

    def x_copy(side, to):
        return remote(
            xs.at[side, to], xr.at[side, e], x_sem.at[0, side], x_sem.at[1, side], expert=to
        )

    def dispatch(side, tok_ref):
        for m in range(micro):
            hot = lax.broadcasted_iota(jnp.int32, (slots_all, tok), 0).astype(F32)
            hot = jnp.where(hot == slot_row[side, m, 0:1, :], 1.0, 0.0).astype(BF16)
            put = jnp.dot(hot, tok_ref[m], preferred_element_type=F32).astype(BF16)
            for to in range(experts):
                xs[side, to, m] = put[to * cap : (to + 1) * cap]
        for k in range(1, experts):
            x_copy(side, (e + k) % experts).start()
        xr[side, e] = xs[side, e]

    def x_landed(side):
        arrive(xr.at[side, pl.ds(1, experts - 1)], x_sem.at[1, side])

    assign(0, routes_ref)
    dispatch(0, tok_own)
    near_mate.start()
    own_in.start()

    counted = jnp.zeros((8, experts), F32)
    summed = jnp.zeros((8, experts), F32)
    present = jnp.zeros((8, 1), F32)
    for m in range(micro):
        logits = lax.dot_general(
            router_ref[...], tok_own[m], (((1,), (1,)), ((), ())), preferred_element_type=F32
        )
        row = routes_ref[m : m + 1, :]
        hot = jnp.where(lax.broadcasted_iota(jnp.int32, (experts, tok), 0) == row, 1.0, 0.0)
        chosen = jnp.sum(logits * hot, axis=0, keepdims=True)
        gate[m] = spread(1.0 / (1.0 + jnp.exp(-chosen)))
        exps = jnp.exp(logits)
        probs = exps / jnp.sum(exps, axis=0, keepdims=True)
        modal = lax.broadcasted_iota(jnp.int32, (8, tok), 0) == modality_ref[m : m + 1, :]
        modal = jnp.where(modal, 1.0, 0.0)
        counted += lax.dot_general(
            modal, hot, (((1,), (1,)), ((), ())),
            precision=lax.Precision.HIGHEST, preferred_element_type=F32,
        )
        summed += lax.dot_general(
            modal, probs, (((1,), (1,)), ((), ())),
            precision=lax.Precision.HIGHEST, preferred_element_type=F32,
        )
        present += jnp.sum(modal, axis=1, keepdims=True)
    sums[0] = jnp.zeros((8, 128), F32)
    sums[0, 0:2, 0:experts] = counted[0:2]
    sums[0, 2:4, 0:experts] = summed[0:2]
    sums[0, 4:6, 0:experts] = jnp.broadcast_to(present[0:2], (2, experts))

    def tell_e(k, carry):
        remote(
            sums.at[0], stats_e.at[e], stat_sem.at[0, 0], stat_sem.at[1, 0], expert=(e + k) % experts
        ).start()
        return carry

    def tell_d(k, carry):
        remote(
            sums.at[1], stats_d.at[p], stat_sem.at[0, 1], stat_sem.at[1, 1], dp=(p + k) % ranks
        ).start()
        return carry

    lax.fori_loop(1, experts, tell_e, 0)
    for i in range(pieces):
        out_mate[i].start()
        own_out[i].start()
    assign_back(0)

    def second_stats():
        arrive(stats_e.at[pl.ds(1, experts - 1)], stat_sem.at[1, 0])
        stats_e[e] = sums[0]
        sums[1] = jnp.sum(stats_e[...], axis=0)
        lax.fori_loop(1, ranks, tell_d, 0)

    half_w = width // 2

    def first_dot(side, which, at, tile):
        left = xr[side, :, :, :, pl.ds(pl.multiple_of(which * half_w, 128), half_w)]
        right = win[pl.ds(pl.multiple_of(which * half_w, 16), half_w), pl.ds(at, tile)]
        return jnp.dot(left.reshape(side_rows, half_w), right, preferred_element_type=F32)

    def near_side(side):
        def near_tile(i, carry):
            at = pl.multiple_of(i * tile, 128)
            acc[side, :, pl.ds(at, tile)] = first_dot(side, h, at, tile)
            return carry

        lax.fori_loop(0, half_ff // tile, near_tile, 0)

    def far_sides(sides, j):
        at = pl.multiple_of(j * far_tile, 128)
        for side in range(sides):
            if side == 2:
                left = xr[side].reshape(side_rows, width)
                pre = jnp.dot(left, win[:, pl.ds(at, far_tile)], preferred_element_type=F32)
            else:
                pre = acc[side, :, pl.ds(at, far_tile)] + first_dot(side, 1 - h, at, far_tile)
            half = 0.5 * pre
            curve = jnp.tanh(pre * (C1 + C3 * (pre * pre)))
            hid[side, :, pl.ds(at, far_tile)] = (half + half * curve).astype(BF16)

    def win_span(blocks, at=0, size=half_ff):
        return win.at[pl.ds(0, blocks * in_rows), pl.ds(at, size)]

    def near_arrived():
        for k in range(1, group):
            arrive(win_rows(peer(k)), near_recv.at[(zl + k) % group])
            pass_near(k).start()

    def near_whole():
        arrive(win_span(group + 1), near_whole_recv)

    def far_arrived(t, which, j):
        q = far_rank(t, which, c)
        arrive(win_rows(q, *chunk(j)), far_recv.at[(q // 2) % group, j])
        pass_far(q, j, 0).start()

    def far_direct(which, j):
        q = far_rank(0, which, c)
        arrive(win_rows(q, *chunk(j)), far_recv.at[(q // 2) % group, j])
        for k in range(1, group):
            pass_far(q, j, k).start()
        pass_far(q, j, 0).start()

    def far_whole(j):
        arrive(win_span(group, *chunk(j)), far_whole_recv.at[j])

    def out_arrived(i):
        for k in range(1, group):
            arrive(wout_rows(place(k, c), i), out_recv.at[(zl + k) % group, i])
            pass_out(k, i).start()

    def out_whole(i):
        span = wout.at[pl.ds(0, (group + 1) * out_rows), pl.ds(i * tile_w, tile_w)]
        arrive(span, out_whole_recv.at[i])

    block = side_rows // 2
    block_e = experts // 2

    def second(i, low, high):
        def step(k, carry):
            side, at = low + k // 2, pl.multiple_of((k % 2) * block, 16)
            got = jnp.dot(
                hid[side, pl.ds(at, block), :],
                wout[:, i * tile_w : (i + 1) * tile_w],
                preferred_element_type=F32,
            )
            if i < direct and low == 0:
                near = w_part[i, pl.ds((k % 2) * block_e, block_e)].reshape(block, tile_w)
                got += jnp.where(inner, near.astype(F32), 0.0)
            got = got.astype(BF16).reshape(block_e, micro, cap, tile_w)
            ys[side, i, pl.ds((k % 2) * block_e, block_e)] = got
            return carry

        lax.fori_loop(0, 2 * (high - low), step, 0)

    def w_copy(i):
        return remote(ys.at[2, i], w_part.at[i], w_send, w_recv.at[i], dp=far_in)

    def y_start(side, i):
        for k in range(1, experts):
            to = (e + k) % experts
            remote(
                ys.at[side, i, to], yr.at[side, i, e], y_send.at[side], y_recv.at[side, i], expert=to
            ).start()
        yr[side, i, e] = ys[side, i, e]

    def y_landed(side, i):
        arrive(yr.at[side, i, pl.ds(1, experts - 1)], y_recv.at[side, i])

    def combine(side, i, m):
        back = yr[side, i, :, m].reshape(slots_all, tile_w)
        return jnp.dot(back_hot[side, m], back, preferred_element_type=F32)

    def z_copy(side, i):
        return remote(
            zs.at[side - 1, i], zr.at[i], z_send.at[side - 1], z_recv.at[i],
            dp=far_out if side == 1 else far_in,
        )

    def give_back(side, i):
        y_landed(side, i)
        for m in range(micro):
            zs[side - 1, i, m] = combine(side, i, m).astype(BF16)
        z_copy(side, i).start()

    @pl.when(inner)
    def _():
        for which in range(2):
            arrive(routes_far.at[which], routes_sem.at[which])
            arrive(tok_far.at[which], tok_sem.at[which])
            assign(1 + which, routes_far.at[which])
            dispatch(1 + which, tok_far.at[which])
            assign_back(1 + which)
            if which == 0:
                for j in range(ahead_parts):
                    far_direct(0, j)
                for i in range(2, early):
                    for copy in out_peers[i]:
                        copy.start()
        second_stats()
        near_arrived()
        x_landed(0)
        near_whole()
        near_side(0)
        for j in range(ahead_parts, ahead_parts + 2):
            far_direct(0, j)
        x_landed(1)
        near_side(1)
        for j in range(ahead_parts + 2, parts):
            far_direct(0, j)

        def far_next(j):
            far_direct(1, j)
            for t in range(1, pairs):
                far_arrived(t, 0, j)
                far_arrived(t, 1, j)

        far_next(0)
        x_landed(2)

        def far_step(j, carry):
            @pl.when(j < parts - 1)
            def _():
                far_next(j + 1)

            @pl.when(j == parts - 2)
            def _():
                for i in range(early, pieces):
                    for copy in out_peers[i]:
                        copy.start()
                out_arrived(0)

            far_whole(j)
            far_sides(3, j)
            return carry

        lax.fori_loop(0, parts, far_step, 0)

        def own(i):
            if i < direct:
                arrive(w_part.at[i], w_recv.at[i])
            second(i, 0, 1)

        def far_piece(i):
            out_whole(i)
            second(i, 1, 2)
            y_start(1, i)
            second(i, 2, 3)
            if i < direct:
                w_copy(i).start()
            else:
                y_start(2, i)

        out_arrived(1)
        far_piece(0)
        far_piece(1)
        for i in range(2, pieces):
            if i == pieces - 1:
                give_back(2, pieces - 3)
            out_arrived(i)
            if i == pieces - 2:
                own(0)
                y_start(0, 0)
            if i == pieces - 1:
                give_back(1, 0)
                own(1)
            far_piece(i)
        y_start(0, 1)
        for i in range(2, pieces):
            own(i)
            y_start(0, i)
            if i == pieces - 3:
                give_back(2, pieces - 2)
        for back in range(1, pieces - 1):
            give_back(1, back)
        give_back(1, pieces - 1)
        give_back(2, pieces - 1)

    @pl.when(outer)
    def _():
        second_stats()
        near_arrived()
        x_landed(0)
        near_whole()
        near_side(0)
        for i in range(early):
            out_arrived(i)

        def far_step(j, carry):
            for t in range(pairs):
                far_arrived(t, 0, j)
                far_arrived(t, 1, j)
            far_whole(j)
            far_sides(1, j)
            return carry

        lax.fori_loop(0, parts, far_step, 0)
        for i in range(pieces):
            if i >= early:
                out_arrived(i)
            out_whole(i)
            second(i, 0, 1)
            y_start(0, i)

    arrive(stats_d.at[pl.ds(1, ranks - 1)], stat_sem.at[1, 1])
    stats_d[p] = sums[1]
    sums[2] = jnp.sum(stats_d[...], axis=0)
    modal_counts = sums[2, 4:6, 0:experts]
    load_ref[0] = experts * sums[2, 0:2, 0:experts] / modal_counts
    load_ref[1] = experts * sums[2, 2:4, 0:experts] / modal_counts

    @pl.when(inner)
    def _():
        for i in range(direct):
            zr[i] = jnp.zeros((micro, tok, tile_w), BF16)

    arrive(stats_e.at[pl.ds(1, experts - 1)], stat_sem.at[0, 0])
    arrive(stats_d.at[pl.ds(1, ranks - 1)], stat_sem.at[0, 1])
    tok_copy.wait_send()
    routes_copy.wait_send()
    arrive(win_span(3 * group), in_send.at[0])
    arrive(wout.at[pl.ds(0, (2 * group - 1) * out_rows), :], out_send)
    arrive(xr.at[0, pl.ds(1, experts - 1)], x_sem.at[0, 0])

    @pl.when(inner)
    def _():
        arrive(win_span(2 * (group - 1)), in_send.at[1])
        for side in (1, 2):
            arrive(xr.at[side, pl.ds(1, experts - 1)], x_sem.at[0, side])
        arrive(yr.at[1, :, pl.ds(1, experts - 1)], y_send.at[1])
        arrive(yr.at[2, pl.ds(direct, pieces - direct), pl.ds(1, experts - 1)], y_send.at[2])
        arrive(w_part, w_send)

    for i in range(pieces):
        y_landed(0, i)
        kept = [combine(0, i, m) for m in range(micro)]
        if i < direct:

            @pl.when(outer)
            def _(i=i):
                arrive(zr.at[i], z_recv.at[i])
        else:
            arrive(zr.at[i], z_recv.at[i])
        for m in range(micro):
            both = kept[m] + zr[i, m].astype(F32)
            scale = jnp.concatenate([gate[m]] * (tile_w // tok), axis=1)
            mixed_ref[m, :, i * tile_w : (i + 1) * tile_w] = (both * scale).astype(BF16)

    arrive(yr.at[0, :, pl.ds(1, experts - 1)], y_send.at[0])

    @pl.when(inner)
    def _():
        arrive(zs.at[0], z_send.at[0])
        arrive(zs.at[1, pl.ds(direct, pieces - direct)], z_send.at[1])


def on_device(tokens, modality, routes, router, w_in, w_out):
    micro, tok, width = tokens.shape
    experts = router.shape[1]
    cap = 2 * tok // experts
    ranks = lax.axis_size("dp")
    group = ranks // 4
    half_ff = w_in.shape[2] // 2
    tile_w = 256 if width % 256 == 0 else 128
    pieces = width // tile_w
    tile = 512 if half_ff % 512 == 0 else 128
    far_tile = 256 if half_ff % 256 == 0 else 128
    parts = half_ff // far_tile

    dma = pltpu.SemaphoreType.DMA
    vmem = pl.BlockSpec(memory_space=pltpu.VMEM)
    hbm = pl.BlockSpec(memory_space=pl.ANY)
    rows = experts * micro * cap
    mixed, load = pl.pallas_call(
        functools.partial(layer_kernel, experts, ranks, tile, far_tile),
        out_shape=(
            pltpu.VMEM(tokens.shape, BF16),
            pltpu.VMEM((2, 2, experts), F32),
        ),
        in_specs=[hbm] + [vmem] * 3 + [hbm] * 2,
        out_specs=(vmem, vmem),
        scratch_shapes=[
            pltpu.VMEM((micro, tok, width), BF16),
            pltpu.VMEM((2, micro, tok, width), BF16),
            pltpu.VMEM((2, micro, tok), jnp.int32),
            pltpu.VMEM((3, micro, 8, tok), F32),
            pltpu.VMEM((3, micro, tok, experts * cap), BF16),
            pltpu.VMEM((micro, tok, tok), F32),
            pltpu.VMEM((3, 8, 128), F32),
            pltpu.VMEM((experts, 8, 128), F32),
            pltpu.VMEM((ranks, 8, 128), F32),
            pltpu.VMEM((width, half_ff), BF16),
            pltpu.VMEM((half_ff, width), BF16),
            pltpu.VMEM((3, experts, micro, cap, width), BF16),
            pltpu.VMEM((3, experts, micro, cap, width), BF16),
            pltpu.VMEM((2, rows, half_ff), F32),
            pltpu.VMEM((3, rows, half_ff), BF16),
            pltpu.VMEM((3, pieces, experts, micro, cap, tile_w), BF16),
            pltpu.VMEM((3, pieces, experts, micro, cap, tile_w), BF16),
            pltpu.VMEM((2, pieces, micro, tok, tile_w), BF16),
            pltpu.VMEM((pieces, micro, tok, tile_w), BF16),
            pltpu.VMEM((2, experts, micro, cap, tile_w), BF16),
            dma((3,)),
            dma((3,)),
            dma((2, 2)),
            dma((2,)),
            dma((group,)),
            dma,
            dma((group, parts)),
            dma((parts,)),
            dma,
            dma((group, pieces)),
            dma((pieces,)),
            dma((2, 3)),
            dma((3,)),
            dma((3, pieces)),
            dma((2,)),
            dma((pieces,)),
            dma,
            dma((2,)),
            dma,
        ],
        compiler_params=pltpu.CompilerParams(
            collective_id=0, has_side_effects=True, vmem_limit_bytes=62 * 1024 * 1024
        ),
    )(tokens, routes[:, :, 0], modality, router.T, w_in[0], w_out[0])
    return (mixed, load)


def solution(mesh):
    placed = (
        P(None, ("expert", "dp"), None),
        P(None, ("expert", "dp")),
        P(None, ("expert", "dp"), None),
        P(),
        P("expert", "dp", None),
        P("expert", "dp", None),
    )
    return jax.shard_map(
        on_device,
        mesh=mesh,
        in_specs=placed,
        out_specs=(P(None, ("expert", "dp"), None), P()),
        check_vma=False,
    )
```

```python
import functools
import math

import jax
import jax.numpy as jnp
from jax import lax
from jax.experimental import pallas as pl
from jax.experimental.pallas import tpu as pltpu
from jax.sharding import PartitionSpec as P

MESH = pl.DeviceIdType.MESH
BF16 = jnp.bfloat16
F32 = jnp.float32
C1 = math.sqrt(2 / math.pi)
C3 = 0.044715 * C1


def layer_kernel(
    experts,
    ranks,
    tile,
    far_tile,
    tokens_ref,
    routes_ref,
    modality_ref,
    router_ref,
    w_in_ref,
    w_out_ref,
    mixed_ref,
    load_ref,
    tok_own,
    tok_far,
    routes_far,
    slot_row,
    back_hot,
    gate,
    sums,
    stats_e,
    stats_d,
    win,
    wout,
    xs,
    xr,
    acc,
    hid,
    ys,
    yr,
    zs,
    zr,
    w_part,
    tok_sem,
    routes_sem,
    stat_sem,
    in_send,
    near_recv,
    near_whole_recv,
    far_recv,
    far_whole_recv,
    out_send,
    out_recv,
    out_whole_recv,
    x_sem,
    y_send,
    y_recv,
    z_send,
    z_recv,
    w_send,
    w_recv,
    load_sem,
):
    micro, tok, width = tokens_ref.shape
    in_rows, ff = w_in_ref.shape
    out_rows = w_out_ref.shape[0]
    half_ff = ff // 2
    pieces, tile_w = zr.shape[0], zr.shape[3]
    direct = w_part.shape[0]
    cap = xs.shape[3]
    slots_all = experts * cap
    side_rows = experts * micro * cap
    e = lax.axis_index("expert")
    p = lax.axis_index("dp")
    z, c = p // 2, p % 2
    chips = ranks // 2
    group = chips // 2
    pairs = group // 2
    h = z // group
    zl = z % group
    mate = z * 2 + (1 - c)
    inner = (z % 2) == (1 - h)
    outer = (z % 2) == h
    role = (z + h) % 2

    def far_rank(t, which, core):
        pair = (1 - h) * pairs + ((z // 2) % pairs + t) % pairs
        return (pair * 2 + (1 - h + which) % 2) * 2 + core

    far_in = far_rank(0, 1, c)
    far_out = far_rank(0, 0, c)

    def peer(k):
        return (h * group + (zl + k) % group) * 2 + c

    def place(k, core):
        return ((zl + k) % group) * 2 + core

    tok_load = pltpu.make_async_copy(tokens_ref, tok_own, load_sem)
    tok_load.start()
    barrier = pltpu.get_barrier_semaphore()

    def greet_e(k, carry):
        pl.semaphore_signal(
            barrier, inc=1, device_id=((e + k) % experts, p), device_id_type=MESH
        )
        return carry

    def greet_d(k, carry):
        pl.semaphore_signal(barrier, inc=1, device_id=(e, (p + k) % ranks), device_id_type=MESH)
        return carry

    lax.fori_loop(1, experts, greet_e, 0)
    lax.fori_loop(1, ranks, greet_d, 0)

    def remote(src, dst, send, recv, dp=None, expert=None):
        return pltpu.make_async_remote_copy(
            src_ref=src,
            dst_ref=dst,
            send_sem=send,
            recv_sem=recv,
            device_id=(e if expert is None else expert, p if dp is None else dp),
            device_id_type=MESH,
        )

    def arrive(ref, sem):
        pltpu.make_async_copy(ref, ref, sem).wait()

    parts = half_ff // far_tile
    ahead_parts = parts * 2 // 5

    def chunk(j):
        at = j * far_tile
        return (at if isinstance(j, int) else pl.multiple_of(at, 128), far_tile)

    def win_rows(q, start=0, size=half_ff):
        return win.at[pl.ds(pl.multiple_of(q * in_rows, 16), in_rows), pl.ds(start, size)]

    def wout_rows(r, piece):
        return wout.at[
            pl.ds(pl.multiple_of(r * out_rows, 16), out_rows), pl.ds(piece * tile_w, tile_w)
        ]

    def cols(which, start=0, size=half_ff):
        return w_in_ref.at[:, pl.ds(pl.multiple_of(which * half_ff + start, 128), size)]

    def w_out_piece(piece):
        return w_out_ref.at[:, pl.ds(piece * tile_w, tile_w)]

    tok_copy = remote(
        tok_own, tok_far.at[role], tok_sem.at[2], tok_sem.at[role], dp=far_in
    )
    routes_copy = remote(
        routes_ref, routes_far.at[role], routes_sem.at[2], routes_sem.at[role], dp=far_in
    )
    far_copies = [
        remote(
            cols(1 - h, *chunk(j)), win_rows(p, *chunk(j)), in_send.at[0], far_recv.at[zl, j], dp=far_in
        )
        for j in range(parts)
    ]
    near_peers = [
        remote(cols(h), win_rows(p), in_send.at[0], near_recv.at[zl], dp=peer(k))
        for k in range(1, group)
    ]
    near_mate = remote(cols(h), win_rows(p), in_send.at[0], near_whole_recv, dp=mate)
    own_in = pltpu.make_async_copy(cols(h), win_rows(p), near_whole_recv)
    mine = place(0, c)
    out_peers = [
        [
            remote(
                w_out_piece(i), wout_rows(mine, i), out_send, out_recv.at[zl, i], dp=peer(k)
            )
            for k in range(1, group)
        ]
        for i in range(pieces)
    ]
    out_mate = [
        remote(
            w_out_piece(i), wout_rows(mine, i), out_send, out_whole_recv.at[i], dp=mate
        )
        for i in range(pieces)
    ]
    own_out = [
        pltpu.make_async_copy(w_out_piece(i), wout_rows(mine, i), out_whole_recv.at[i])
        for i in range(pieces)
    ]

    def pass_near(k):
        q = peer(k)
        return remote(win_rows(q), win_rows(q), in_send.at[0], near_whole_recv, dp=mate)

    def pass_far(q, j, k):
        rows = win_rows(q, *chunk(j))
        if k == 0:
            return remote(rows, rows, in_send.at[0], far_whole_recv.at[j], dp=mate)
        at = (q // 2) % group
        return remote(rows, rows, in_send.at[1], far_recv.at[at, j], dp=peer(k))

    def pass_out(k, i):
        r = place(k, c)
        rows = wout_rows(r, i)
        return remote(rows, rows, out_send, out_whole_recv.at[i], dp=mate)

    tok_load.wait()
    pl.semaphore_wait(barrier, experts + ranks - 2)

    early = pieces - 2
    routes_copy.start()
    tok_copy.start()

    @pl.when(inner)
    def _():
        for copy in far_copies:
            copy.start()
        for copy in near_peers:
            copy.start()
        for i in range(2):
            for copy in out_peers[i]:
                copy.start()

    @pl.when(outer)
    def _():
        for copy in far_copies[:ahead_parts]:
            copy.start()
        for copy in near_peers:
            copy.start()
        for copy in far_copies[ahead_parts:]:
            copy.start()
        for i in range(pieces):
            for copy in out_peers[i]:
                copy.start()


    rows_e = max(experts, 8)

    def hot_of(row):
        at = lax.broadcasted_iota(jnp.int32, (rows_e, tok), 0)
        return jnp.where(at == row, 1.0, 0.0)

    def spread(row):
        return jnp.broadcast_to(row, (tok, tok)).T

    def assign(side, ref):
        ahead = lax.broadcasted_iota(jnp.int32, (tok, tok), 0) < lax.broadcasted_iota(
            jnp.int32, (tok, tok), 1
        )
        ahead = jnp.where(ahead, 1.0, 0.0).astype(BF16)
        for m in range(micro):
            row = ref[m : m + 1, :]
            hot = hot_of(row)
            before = jnp.dot(hot.astype(BF16), ahead, preferred_element_type=F32)
            slot = jnp.sum(hot * before, axis=0, keepdims=True) + row.astype(F32) * cap
            slot_row[side, m] = jnp.broadcast_to(slot, (8, tok))

    def assign_back(side):
        lanes = lax.broadcasted_iota(jnp.int32, (tok, slots_all), 1).astype(F32)
        for m in range(micro):
            slot = spread(slot_row[side, m, 0:1, :])
            wide = jnp.concatenate([slot] * (slots_all // tok), axis=1)
            back_hot[side, m] = jnp.where(lanes == wide, 1.0, 0.0).astype(BF16)

    def x_copy(side, to):
        return remote(
            xs.at[side, to], xr.at[side, e], x_sem.at[0, side], x_sem.at[1, side], expert=to
        )

    def dispatch(side, tok_ref):
        for m in range(micro):
            hot = lax.broadcasted_iota(jnp.int32, (slots_all, tok), 0).astype(F32)
            hot = jnp.where(hot == slot_row[side, m, 0:1, :], 1.0, 0.0).astype(BF16)
            put = jnp.dot(hot, tok_ref[m], preferred_element_type=F32).astype(BF16)
            for to in range(experts):
                xs[side, to, m] = put[to * cap : (to + 1) * cap]
        for k in range(1, experts):
            x_copy(side, (e + k) % experts).start()
        xr[side, e] = xs[side, e]

    def x_landed(side):
        arrive(xr.at[side, pl.ds(1, experts - 1)], x_sem.at[1, side])

    assign(0, routes_ref)
    dispatch(0, tok_own)
    near_mate.start()
    own_in.start()

    counted = jnp.zeros((8, experts), F32)
    summed = jnp.zeros((8, experts), F32)
    present = jnp.zeros((8, 1), F32)
    for m in range(micro):
        logits = lax.dot_general(
            router_ref[...], tok_own[m], (((1,), (1,)), ((), ())), preferred_element_type=F32
        )
        row = routes_ref[m : m + 1, :]
        hot = jnp.where(lax.broadcasted_iota(jnp.int32, (experts, tok), 0) == row, 1.0, 0.0)
        chosen = jnp.sum(logits * hot, axis=0, keepdims=True)
        gate[m] = spread(1.0 / (1.0 + jnp.exp(-chosen)))
        exps = jnp.exp(logits)
        probs = exps / jnp.sum(exps, axis=0, keepdims=True)
        modal = lax.broadcasted_iota(jnp.int32, (8, tok), 0) == modality_ref[m : m + 1, :]
        modal = jnp.where(modal, 1.0, 0.0)
        counted += lax.dot_general(
            modal, hot, (((1,), (1,)), ((), ())),
            precision=lax.Precision.HIGHEST, preferred_element_type=F32,
        )
        summed += lax.dot_general(
            modal, probs, (((1,), (1,)), ((), ())),
            precision=lax.Precision.HIGHEST, preferred_element_type=F32,
        )
        present += jnp.sum(modal, axis=1, keepdims=True)
    sums[0] = jnp.zeros((8, 128), F32)
    sums[0, 0:2, 0:experts] = counted[0:2]
    sums[0, 2:4, 0:experts] = summed[0:2]
    sums[0, 4:6, 0:experts] = jnp.broadcast_to(present[0:2], (2, experts))

    def tell_e(k, carry):
        remote(
            sums.at[0], stats_e.at[e], stat_sem.at[0, 0], stat_sem.at[1, 0], expert=(e + k) % experts
        ).start()
        return carry

    def tell_d(k, carry):
        remote(
            sums.at[1], stats_d.at[p], stat_sem.at[0, 1], stat_sem.at[1, 1], dp=(p + k) % ranks
        ).start()
        return carry

    lax.fori_loop(1, experts, tell_e, 0)
    for i in range(pieces):
        out_mate[i].start()
        own_out[i].start()
    assign_back(0)

    def second_stats():
        arrive(stats_e.at[pl.ds(1, experts - 1)], stat_sem.at[1, 0])
        stats_e[e] = sums[0]
        sums[1] = jnp.sum(stats_e[...], axis=0)
        lax.fori_loop(1, ranks, tell_d, 0)

    half_w = width // 2

    def first_dot(side, which, at, tile):
        left = xr[side, :, :, :, pl.ds(pl.multiple_of(which * half_w, 128), half_w)]
        right = win[pl.ds(pl.multiple_of(which * half_w, 16), half_w), pl.ds(at, tile)]
        return jnp.dot(left.reshape(side_rows, half_w), right, preferred_element_type=F32)

    def near_side(side):
        def near_tile(i, carry):
            at = pl.multiple_of(i * tile, 128)
            acc[side, :, pl.ds(at, tile)] = first_dot(side, h, at, tile)
            return carry

        lax.fori_loop(0, half_ff // tile, near_tile, 0)

    def far_sides(sides, j):
        at = pl.multiple_of(j * far_tile, 128)
        for side in range(sides):
            if side == 2:
                left = xr[side].reshape(side_rows, width)
                pre = jnp.dot(left, win[:, pl.ds(at, far_tile)], preferred_element_type=F32)
            else:
                pre = acc[side, :, pl.ds(at, far_tile)] + first_dot(side, 1 - h, at, far_tile)
            half = 0.5 * pre
            curve = jnp.tanh(pre * (C1 + C3 * (pre * pre)))
            hid[side, :, pl.ds(at, far_tile)] = (half + half * curve).astype(BF16)

    def win_span(blocks, at=0, size=half_ff):
        return win.at[pl.ds(0, blocks * in_rows), pl.ds(at, size)]

    def near_arrived():
        for k in range(1, group):
            arrive(win_rows(peer(k)), near_recv.at[(zl + k) % group])
            pass_near(k).start()

    def near_whole():
        arrive(win_span(group + 1), near_whole_recv)

    def far_arrived(t, which, j):
        q = far_rank(t, which, c)
        arrive(win_rows(q, *chunk(j)), far_recv.at[(q // 2) % group, j])
        pass_far(q, j, 0).start()

    def far_direct(which, j):
        q = far_rank(0, which, c)
        arrive(win_rows(q, *chunk(j)), far_recv.at[(q // 2) % group, j])
        for k in range(1, group):
            pass_far(q, j, k).start()
        pass_far(q, j, 0).start()

    def far_whole(j):
        arrive(win_span(group, *chunk(j)), far_whole_recv.at[j])

    def out_arrived(i):
        for k in range(1, group):
            arrive(wout_rows(place(k, c), i), out_recv.at[(zl + k) % group, i])
            pass_out(k, i).start()

    def out_whole(i):
        span = wout.at[pl.ds(0, (group + 1) * out_rows), pl.ds(i * tile_w, tile_w)]
        arrive(span, out_whole_recv.at[i])

    block = side_rows // 2
    block_e = experts // 2

    def second(i, low, high):
        def step(k, carry):
            side, at = low + k // 2, pl.multiple_of((k % 2) * block, 16)
            got = jnp.dot(
                hid[side, pl.ds(at, block), :],
                wout[:, i * tile_w : (i + 1) * tile_w],
                preferred_element_type=F32,
            )
            if i < direct and low == 0:
                near = w_part[i, pl.ds((k % 2) * block_e, block_e)].reshape(block, tile_w)
                got += jnp.where(inner, near.astype(F32), 0.0)
            got = got.astype(BF16).reshape(block_e, micro, cap, tile_w)
            ys[side, i, pl.ds((k % 2) * block_e, block_e)] = got
            return carry

        lax.fori_loop(0, 2 * (high - low), step, 0)

    def w_copy(i):
        return remote(ys.at[2, i], w_part.at[i], w_send, w_recv.at[i], dp=far_in)

    def y_start(side, i):
        for k in range(1, experts):
            to = (e + k) % experts
            remote(
                ys.at[side, i, to], yr.at[side, i, e], y_send.at[side], y_recv.at[side, i], expert=to
            ).start()
        yr[side, i, e] = ys[side, i, e]

    def y_landed(side, i):
        arrive(yr.at[side, i, pl.ds(1, experts - 1)], y_recv.at[side, i])

    def combine(side, i, m):
        back = yr[side, i, :, m].reshape(slots_all, tile_w)
        return jnp.dot(back_hot[side, m], back, preferred_element_type=F32)

    def z_copy(side, i):
        return remote(
            zs.at[side - 1, i], zr.at[i], z_send.at[side - 1], z_recv.at[i],
            dp=far_out if side == 1 else far_in,
        )

    def give_back(side, i):
        y_landed(side, i)
        for m in range(micro):
            zs[side - 1, i, m] = combine(side, i, m).astype(BF16)
        z_copy(side, i).start()

    @pl.when(inner)
    def _():
        for which in range(2):
            arrive(routes_far.at[which], routes_sem.at[which])
            arrive(tok_far.at[which], tok_sem.at[which])
            assign(1 + which, routes_far.at[which])
            dispatch(1 + which, tok_far.at[which])
            assign_back(1 + which)
            if which == 0:
                for j in range(ahead_parts):
                    far_direct(0, j)
                for i in range(2, early):
                    for copy in out_peers[i]:
                        copy.start()
        second_stats()
        near_arrived()
        x_landed(0)
        near_whole()
        near_side(0)
        for j in range(ahead_parts, ahead_parts + 2):
            far_direct(0, j)
        x_landed(1)
        near_side(1)
        for j in range(ahead_parts + 2, parts):
            far_direct(0, j)

        def far_next(j):
            far_direct(1, j)
            for t in range(1, pairs):
                far_arrived(t, 0, j)
                far_arrived(t, 1, j)

        far_next(0)
        x_landed(2)

        def far_step(j, carry):
            @pl.when(j < parts - 1)
            def _():
                far_next(j + 1)

            @pl.when(j == parts - 2)
            def _():
                for i in range(early, pieces):
                    for copy in out_peers[i]:
                        copy.start()
                out_arrived(0)

            far_whole(j)
            far_sides(3, j)
            return carry

        lax.fori_loop(0, parts, far_step, 0)

        def own(i):
            if i < direct:
                arrive(w_part.at[i], w_recv.at[i])
            second(i, 0, 1)

        def far_piece(i):
            out_whole(i)
            second(i, 1, 2)
            y_start(1, i)
            second(i, 2, 3)
            if i < direct:
                w_copy(i).start()
            else:
                y_start(2, i)

        out_arrived(1)
        far_piece(0)
        far_piece(1)
        for i in range(2, pieces):
            if i == pieces - 2:
                own(0)
                y_start(0, 0)
            if i == pieces - 1:
                give_back(2, pieces - 3)
                own(1)
                y_start(0, 1)
            out_arrived(i)
            if i == pieces - 1:
                give_back(1, 0)
            far_piece(i)
        for back in range(1, pieces - 2):
            give_back(1, back)
        for i in range(2, pieces):
            own(i)
            y_start(0, i)
            if i == pieces - 3:
                give_back(2, pieces - 2)
            if i == pieces - 2:
                give_back(1, pieces - 2)
        give_back(1, pieces - 1)
        give_back(2, pieces - 1)

    @pl.when(outer)
    def _():
        second_stats()
        near_arrived()
        x_landed(0)
        near_whole()
        near_side(0)
        for i in range(early):
            out_arrived(i)

        def far_step(j, carry):
            for t in range(pairs):
                far_arrived(t, 0, j)
                far_arrived(t, 1, j)
            far_whole(j)
            far_sides(1, j)
            return carry

        lax.fori_loop(0, parts, far_step, 0)
        for i in range(pieces):
            if i >= early:
                out_arrived(i)
            out_whole(i)
            second(i, 0, 1)
            y_start(0, i)

    arrive(stats_d.at[pl.ds(1, ranks - 1)], stat_sem.at[1, 1])
    stats_d[p] = sums[1]
    sums[2] = jnp.sum(stats_d[...], axis=0)
    modal_counts = sums[2, 4:6, 0:experts]
    load_ref[0] = experts * sums[2, 0:2, 0:experts] / modal_counts
    load_ref[1] = experts * sums[2, 2:4, 0:experts] / modal_counts

    @pl.when(inner)
    def _():
        for i in range(direct):
            zr[i] = jnp.zeros((micro, tok, tile_w), BF16)

    arrive(stats_e.at[pl.ds(1, experts - 1)], stat_sem.at[0, 0])
    arrive(stats_d.at[pl.ds(1, ranks - 1)], stat_sem.at[0, 1])
    tok_copy.wait_send()
    routes_copy.wait_send()
    arrive(win_span(3 * group), in_send.at[0])
    arrive(wout.at[pl.ds(0, (2 * group - 1) * out_rows), :], out_send)
    arrive(xr.at[0, pl.ds(1, experts - 1)], x_sem.at[0, 0])

    @pl.when(inner)
    def _():
        arrive(win_span(2 * (group - 1)), in_send.at[1])
        for side in (1, 2):
            arrive(xr.at[side, pl.ds(1, experts - 1)], x_sem.at[0, side])
        arrive(yr.at[1, :, pl.ds(1, experts - 1)], y_send.at[1])
        arrive(yr.at[2, pl.ds(direct, pieces - direct), pl.ds(1, experts - 1)], y_send.at[2])
        arrive(w_part, w_send)

    for i in range(pieces):
        y_landed(0, i)
        kept = [combine(0, i, m) for m in range(micro)]
        if i < direct:

            @pl.when(outer)
            def _(i=i):
                arrive(zr.at[i], z_recv.at[i])
        else:
            arrive(zr.at[i], z_recv.at[i])
        for m in range(micro):
            both = kept[m] + zr[i, m].astype(F32)
            scale = jnp.concatenate([gate[m]] * (tile_w // tok), axis=1)
            mixed_ref[m, :, i * tile_w : (i + 1) * tile_w] = (both * scale).astype(BF16)

    arrive(yr.at[0, :, pl.ds(1, experts - 1)], y_send.at[0])

    @pl.when(inner)
    def _():
        arrive(zs.at[0], z_send.at[0])
        arrive(zs.at[1, pl.ds(direct, pieces - direct)], z_send.at[1])


def on_device(tokens, modality, routes, router, w_in, w_out):
    micro, tok, width = tokens.shape
    experts = router.shape[1]
    cap = 2 * tok // experts
    ranks = lax.axis_size("dp")
    group = ranks // 4
    half_ff = w_in.shape[2] // 2
    tile_w = 256 if width % 256 == 0 else 128
    pieces = width // tile_w
    tile = 512 if half_ff % 512 == 0 else 128
    far_tile = 256 if half_ff % 256 == 0 else 128
    parts = half_ff // far_tile

    dma = pltpu.SemaphoreType.DMA
    vmem = pl.BlockSpec(memory_space=pltpu.VMEM)
    hbm = pl.BlockSpec(memory_space=pl.ANY)
    rows = experts * micro * cap
    mixed, load = pl.pallas_call(
        functools.partial(layer_kernel, experts, ranks, tile, far_tile),
        out_shape=(
            pltpu.VMEM(tokens.shape, BF16),
            pltpu.VMEM((2, 2, experts), F32),
        ),
        in_specs=[hbm] + [vmem] * 3 + [hbm] * 2,
        out_specs=(vmem, vmem),
        scratch_shapes=[
            pltpu.VMEM((micro, tok, width), BF16),
            pltpu.VMEM((2, micro, tok, width), BF16),
            pltpu.VMEM((2, micro, tok), jnp.int32),
            pltpu.VMEM((3, micro, 8, tok), F32),
            pltpu.VMEM((3, micro, tok, experts * cap), BF16),
            pltpu.VMEM((micro, tok, tok), F32),
            pltpu.VMEM((3, 8, 128), F32),
            pltpu.VMEM((experts, 8, 128), F32),
            pltpu.VMEM((ranks, 8, 128), F32),
            pltpu.VMEM((width, half_ff), BF16),
            pltpu.VMEM((half_ff, width), BF16),
            pltpu.VMEM((3, experts, micro, cap, width), BF16),
            pltpu.VMEM((3, experts, micro, cap, width), BF16),
            pltpu.VMEM((2, rows, half_ff), F32),
            pltpu.VMEM((3, rows, half_ff), BF16),
            pltpu.VMEM((3, pieces, experts, micro, cap, tile_w), BF16),
            pltpu.VMEM((3, pieces, experts, micro, cap, tile_w), BF16),
            pltpu.VMEM((2, pieces, micro, tok, tile_w), BF16),
            pltpu.VMEM((pieces, micro, tok, tile_w), BF16),
            pltpu.VMEM((2, experts, micro, cap, tile_w), BF16),
            dma((3,)),
            dma((3,)),
            dma((2, 2)),
            dma((2,)),
            dma((group,)),
            dma,
            dma((group, parts)),
            dma((parts,)),
            dma,
            dma((group, pieces)),
            dma((pieces,)),
            dma((2, 3)),
            dma((3,)),
            dma((3, pieces)),
            dma((2,)),
            dma((pieces,)),
            dma,
            dma((2,)),
            dma,
        ],
        compiler_params=pltpu.CompilerParams(
            collective_id=0, has_side_effects=True, vmem_limit_bytes=62 * 1024 * 1024
        ),
    )(tokens, routes[:, :, 0], modality, router.T, w_in[0], w_out[0])
    return (mixed, load)


def solution(mesh):
    placed = (
        P(None, ("expert", "dp"), None),
        P(None, ("expert", "dp")),
        P(None, ("expert", "dp"), None),
        P(),
        P("expert", "dp", None),
        P("expert", "dp", None),
    )
    return jax.shard_map(
        on_device,
        mesh=mesh,
        in_specs=placed,
        out_specs=(P(None, ("expert", "dp"), None), P()),
        check_vma=False,
    )
```
